32 devices in a mesh: dp: 8 (over z, x), expert: 4 (over y, core).
Axes of the slice: x: 2, y: 2, z: 4, core: 2. Of those that a mesh axis runs over, the one named last changes fastest.
Arguments:
- queries: bfloat16 [256, 2048], P(('dp', 'expert')), may hold values from -8 to 8
- fresh_key: bfloat16 [256, 256], P(('dp', 'expert')), may hold values from -4 to 4
- fresh_value: bfloat16 [256, 256], P(('dp', 'expert')), may hold values from -4 to 4
- cached_keys: bfloat16 [256, 128, 256], P(('dp', 'expert')), may hold values from -8 to 8
- cached_values: bfloat16 [256, 128, 256], P(('dp', 'expert')), may hold values from -4 to 4
- lengths: int32 [256], P(('dp', 'expert')), may hold values from 2 to 128
- sink_logit_rows: float32 [32], replicated, may hold values from 1 to 5
- residual: bfloat16 [256, 2880], P('dp', 'expert'), may hold values from -6 to 6
- o_weight: bfloat16 [2880, 2048], P('expert'), may hold values from -0.125 to 0.125
- norm_gain: float32 [2880], replicated, may hold values from 0.5 to 1.5
- expert_ids: int32 [256, 4], replicated, may hold values from 0 to 7, all different within a row; in each aligned block of 32 rows (0 to 31, 32 to 63, ...) at most 32 rows name the same one
- route_weights: float32 [256, 4], replicated, may hold values from 0.1 to 0.6
- w_gate_up: bfloat16 [8, 2, 2880, 2880], P('dp', None, 'expert'), may hold values from -0.109375 to 0.109375
- w_down: bfloat16 [8, 2880, 2880], P('dp', 'expert'), may hold values from -0.15625 to 0.15625
Outputs:
- layer_out: bfloat16 [256, 2880], P('dp', 'expert')
The draws below stay inside these ranges and needn't reach their ends.
Inputs may be any that keep to these rules, and one draw needn't show every extreme that they name: `expert_ids`: each row names 4 different experts; among any aligned block of 32 rows no expert is named by more than 32 rows.
All inputs are finite; a program needn't handle non-finite values.
Results may differ from the reference program's by a relative error of at most 0.018.
Values may be sent and summed in bfloat16 or wider, within the bound.
No kernel may reach another device: no remote copies, remote signals or barrier semaphores. Data moves between devices by JAX's collectives and lax.ppermute only.
A program may use at most 64 MiB of HBM per device.

```python
import math
import jax
import jax.numpy as jnp
import numpy as np
from jax import lax

D = 2880
FF = 2880
QUERY_HEADS = 32
KEY_VALUE_HEADS = 4
HEAD_SIZE = 64
WINDOW_LENGTH = 128
TOP = 4
TOK_GROUP = 32
BATCH_ROWS = 256
EXPERTS = 8
CAP = 32
N_DP = 8
N_EXPERT = 4


def draw_queries(key, part):
    own = jax.random.fold_in(key, 11)
    base = jax.random.truncated_normal(own, -4.0, 4.0, (BATCH_ROWS, QUERY_HEADS * HEAD_SIZE), jnp.float32)
    return base.astype(jnp.bfloat16)


def draw_cached_keys(key, part):
    own = jax.random.fold_in(key, 13)
    array_shape = (BATCH_ROWS, WINDOW_LENGTH, KEY_VALUE_HEADS * HEAD_SIZE)
    base = jax.random.truncated_normal(own, -4.0, 4.0, array_shape, jnp.float32)
    return base.astype(jnp.bfloat16)


def set_ends(values, key, low, top_value):
    spot = [jax.random.randint(jax.random.fold_in(key, axis), (), 0, length) for axis, length in enumerate(values.shape)]
    main_axis = values.shape.index(max(values.shape))
    next_to = spot[:main_axis] + [(spot[main_axis] + 1) % values.shape[main_axis]] + spot[main_axis + 1:]
    return values.at[tuple(spot)].set(low).at[tuple(next_to)].set(top_value)


def raised(result, key, source, target, blocks, factor):
    def block_of(position):
        return (jnp.arange(result.shape[position]) // (result.shape[position] // blocks)).reshape((-1,) + (1,) * (result.ndim - 1 - position))

    near = jax.random.permutation(key, blocks)[block_of(target)]
    other_side = (block_of(target) + blocks // 2) % blocks
    return jnp.where((block_of(source) == near) | (block_of(source) == other_side), factor * result, result)


def level_of(own_key, dims, shards, low, largest):
    loudness = 1.0
    for dim, blocks in shards:
        steps = jax.random.uniform(jax.random.fold_in(jax.random.fold_in(own_key, 6), dim), (blocks,), jnp.float32, low / len(shards), largest / len(shards))
        loudness = loudness * jnp.repeat(jnp.exp(steps), dims[dim] // blocks).reshape((-1,) + (1,) * (len(dims) - 1 - dim))
    return loudness


def deal_out(rng, own, number, rows, number_of, top, bound, slope):
    order = jax.random.permutation(rng, number_of)
    crowded, common = load_shares(number_of, rows * top, bound, slope, True), load_shares(number_of, rows * top, bound, slope, False)
    places = jnp.arange(number_of)

    def named(tallies, offset_by):
        used = int((tallies > 0).sum())
        fixed = max(1, used // 4)
        moved = fixed + (places - fixed + offset_by * (used - fixed)) % max(1, number_of - fixed)
        return jnp.zeros((number_of,), jnp.int32).at[order[jnp.where(places < fixed, places, moved)]].set(jnp.asarray(tallies, jnp.int32))

    tallies = jnp.where(number % 4 == 0, named(crowded, number // 4), named(common, number - number // 4 - 1))
    mixed = jax.random.permutation(jax.random.fold_in(own, 3), number_of)
    donor, receiver = mixed[0:number_of // 2 * 2:2], mixed[1:number_of // 2 * 2:2]
    slack = jnp.minimum(tallies[donor] - 1, bound - tallies[receiver]) // 2
    slack = jnp.where((donor == order[0]) | (receiver == order[0]) | (tallies[receiver] == 0), 0, jnp.maximum(slack, 0))
    moved = jax.random.randint(jax.random.fold_in(own, 4), (number_of // 2,), 0, 1 << 20) % (slack + 1)
    tallies = tallies.at[donor].add(-moved).at[receiver].add(moved)
    labels = jnp.searchsorted(jnp.cumsum(tallies), jnp.arange(rows * top), side="right").astype(jnp.int32)
    listing = labels.reshape(top, rows).T
    listing = listing[jax.random.permutation(jax.random.fold_in(own, 1), rows)]
    offset_by = jax.random.randint(jax.random.fold_in(own, 2), (rows, 1), 0, top)
    return jnp.take_along_axis(listing, (jnp.arange(top)[None, :] + offset_by) % top, axis=1)


def load_shares(amount, total, most, slope, full):
    weights = [(1 << 20) // math.isqrt(grade ** slope) + 1 for grade in range(1, amount + 1)]
    largest = most if full else min(most, max(-(-total // amount), total * weights[0] // sum(weights)))
    least = 1 if total - largest >= amount - 1 else 0
    given, surplus = [largest] + [least] * (amount - 1), total - largest - least * (amount - 1)
    while surplus > 0:
        movable = [i for i in range(1, amount) if given[i] < largest] or [i for i in range(1, amount) if given[i] < most]
        pool, left = sum([weights[i] for i in movable]), surplus
        for i in movable:
            addition = min(most - given[i], max(1, left * weights[i] // pool), surplus)
            given[i] = given[i] + addition
            surplus = surplus - addition
    return np.array(given)


def scatter_about(stream_key, dims, scale, most, cuts=(), kind=jnp.bfloat16):
    entries = jax.random.normal(stream_key, dims, jnp.float32) * scale
    if len(cuts) > 0:
        entries = level_of(stream_key, dims, cuts, -0.22, 0.18) * entries
    return jnp.clip(entries, min=-most, max=most).astype(kind)


def bell_draw_with(rng, shape, deviation, bound, pieces, heavy, held_as=jnp.bfloat16):
    drawn = deviation * jax.random.normal(rng, shape, jnp.float32)
    if pieces:
        drawn = drawn * level_of(rng, shape, pieces, -0.22, 0.18)
    return jnp.clip(raised(drawn, jax.random.fold_in(rng, 3), *heavy), -bound, bound).astype(held_as)


def setup_inputs(seed: int = 0) -> dict:
    key_of = jax.random.split(jax.random.key(seed), 15)
    queries = draw_queries(jax.random.fold_in(key_of[14], 71), 0)
    fresh_key = scatter_about(key_of[1], (BATCH_ROWS, KEY_VALUE_HEADS * HEAD_SIZE), 1.0, 4.0, ((0, 32),))
    fresh_value = scatter_about(key_of[2], (BATCH_ROWS, KEY_VALUE_HEADS * HEAD_SIZE), 1.0, 4.0, ((0, 32),))
    cached_keys = draw_cached_keys(jax.random.fold_in(key_of[14], 71), 0)
    cached_values = scatter_about(key_of[4], (BATCH_ROWS, WINDOW_LENGTH, KEY_VALUE_HEADS * HEAD_SIZE), 1.0, 4.0, ((0, 32),))
    lengths = set_ends(jax.random.randint(key_of[5], (BATCH_ROWS,), 2, WINDOW_LENGTH + 1), jax.random.fold_in(key_of[5], 1), 2, WINDOW_LENGTH).astype(jnp.int32)
    sink_logit_rows = jnp.clip(jax.random.uniform(key_of[6], (QUERY_HEADS,), jnp.float32, 1.0, 5.0), 1.0, 5.0)
    residual = scatter_about(key_of[7], (BATCH_ROWS, D), 1.0, 6.0, ((0, 8), (1, 4)))
    o_weight = scatter_about(key_of[8], (D, QUERY_HEADS * HEAD_SIZE), (QUERY_HEADS * HEAD_SIZE) ** -0.5, 0.125, ((0, 4),))
    norm_gain = jnp.clip(1.0 + 0.1 * jax.random.normal(key_of[9], (D,), jnp.float32), 0.5, 1.5)
    expert_ids_keys = jax.random.split(jax.random.fold_in(key_of[10], 1), BATCH_ROWS // TOK_GROUP)
    expert_ids_turns = jax.random.permutation(jax.random.fold_in(key_of[10], 3), BATCH_ROWS // TOK_GROUP)
    expert_ids = jax.vmap(lambda own, number: deal_out(jax.random.fold_in(key_of[10], 2), own, number, TOK_GROUP, EXPERTS, TOP, CAP, 2))(expert_ids_keys, expert_ids_turns).reshape((BATCH_ROWS, TOP))
    route_weights = jnp.clip(jax.random.uniform(key_of[11], (BATCH_ROWS, TOP), jnp.float32, 0.1, 0.6), 0.1, 0.6)
    w_gate_up = scatter_about(key_of[12], (EXPERTS, 2, FF, D), D ** -0.5, 0.109375, ((0, 8), (2, 4)))
    w_down = bell_draw_with(key_of[13], (EXPERTS, FF, D), FF ** -0.5, 0.15625, ((0, 8), (1, 4)), (1, 2, 4, 2.0))
    return dict(queries=queries, fresh_key=fresh_key, fresh_value=fresh_value, cached_keys=cached_keys, cached_values=cached_values, lengths=lengths, sink_logit_rows=sink_logit_rows, residual=residual, o_weight=o_weight, norm_gain=norm_gain, expert_ids=expert_ids, route_weights=route_weights, w_gate_up=w_gate_up, w_down=w_down)


norm_eps = 1e-05
swish_alpha = 1.702

def attend(queries, fresh_key, fresh_value, cached_keys, cached_values, lengths, sink_logit_rows):
    batch_count = queries.shape[0]
    head_groups = QUERY_HEADS // KEY_VALUE_HEADS
    query_head_rows = queries.reshape(batch_count, KEY_VALUE_HEADS, head_groups, HEAD_SIZE).astype(jnp.float32)
    key_rows = cached_keys.reshape(batch_count, WINDOW_LENGTH, KEY_VALUE_HEADS, HEAD_SIZE).astype(jnp.float32)
    value_rows = cached_values.reshape(batch_count, WINDOW_LENGTH, KEY_VALUE_HEADS, HEAD_SIZE).astype(jnp.float32)
    score_scale = 1.0 / math.sqrt(HEAD_SIZE)
    cache_scores = jnp.einsum('bkgd,bwkd->bkgw', query_head_rows, key_rows) * score_scale
    own_scores = jnp.einsum('npwm,npm->npw', query_head_rows, fresh_key.reshape(batch_count, KEY_VALUE_HEADS, HEAD_SIZE).astype(jnp.float32)) * score_scale
    slots = jnp.arange(WINDOW_LENGTH, dtype=jnp.int32)
    valid = (slots[None, :] >= (WINDOW_LENGTH - lengths)[:, None])[:, None, None, :]
    sink_terms = sink_logit_rows.reshape(KEY_VALUE_HEADS, head_groups)[None]
    masked = jnp.where(valid, cache_scores, -jnp.inf)
    top = jnp.maximum(jnp.maximum(lax.optimization_barrier(jnp.max(masked, axis=-1)), own_scores), sink_terms)
    cache_exp = jnp.where(valid, jnp.exp(masked - top[..., None]), 0.0)
    self_exp = jnp.exp(own_scores - top)
    total = lax.optimization_barrier(jnp.sum(cache_exp, axis=-1)) + self_exp + jnp.exp(sink_terms - top)
    cache_prob = (cache_exp / total[..., None]).astype(jnp.bfloat16)
    own_probability = (self_exp / total).astype(jnp.bfloat16)
    blended = jnp.einsum('bkgw,bwkd->bkgd', cache_prob.astype(jnp.float32), value_rows)
    blended = blended + own_probability.astype(jnp.float32)[..., None] * fresh_value.reshape(batch_count, KEY_VALUE_HEADS, 1, HEAD_SIZE).astype(jnp.float32)
    return blended.reshape(batch_count, QUERY_HEADS * HEAD_SIZE).astype(jnp.bfloat16)

def reference(queries, fresh_key, fresh_value, cached_keys, cached_values, lengths, sink_logit_rows, residual, o_weight, norm_gain, expert_ids, route_weights, w_gate_up, w_down):
    attended = attend(queries, fresh_key, fresh_value, cached_keys, cached_values, lengths, sink_logit_rows)
    projected = jnp.dot(attended, o_weight.T, preferred_element_type=jnp.float32)
    stream = (residual.astype(jnp.float32) + projected).astype(jnp.bfloat16)
    wide = stream.astype(jnp.float32)
    score_scale = lax.rsqrt(lax.optimization_barrier(jnp.mean(wide * wide, axis=1, keepdims=True)) + norm_eps)
    normed = (wide * score_scale * norm_gain[None, :]).astype(jnp.bfloat16)
    rows_all = EXPERTS * CAP
    block_hidden = FF // N_EXPERT
    padded = jnp.concatenate([normed, jnp.zeros((1, D), jnp.bfloat16)], axis=0)
    tokens = jnp.arange(BATCH_ROWS, dtype=jnp.int32)
    blocks = jnp.arange(N_DP, dtype=jnp.int32)

    def visit(total, expert):
        picked = expert_ids == expert
        named = jnp.any(picked, axis=1).astype(jnp.int32)
        weight_at = lax.optimization_barrier(jnp.sum(jnp.where(picked, route_weights, 0.0), axis=1))
        ranks = jnp.cumsum(named.reshape(N_DP, TOK_GROUP), axis=1) - 1
        slot = (blocks[:, None] * CAP + ranks).reshape(BATCH_ROWS)
        slot = jnp.where(named > 0, slot, rows_all).astype(jnp.int32)
        source = jnp.full((rows_all + 1,), BATCH_ROWS, jnp.int32).at[slot].set(tokens)[:rows_all]
        inputs = padded[source]
        gate = jnp.dot(inputs, w_gate_up[expert, 0].T, preferred_element_type=jnp.float32)
        up = jnp.dot(inputs, w_gate_up[expert, 1].T, preferred_element_type=jnp.float32)
        hidden = ((up + 1.0) * gate * jax.nn.sigmoid(swish_alpha * gate)).astype(jnp.bfloat16)
        parts = jnp.einsum('rnf,nfd->rnd', hidden.reshape(rows_all, N_EXPERT, block_hidden).astype(jnp.float32), w_down[expert].reshape(N_EXPERT, block_hidden, D).astype(jnp.float32))
        rounded = lax.optimization_barrier(parts.astype(jnp.bfloat16))
        expert_out = lax.optimization_barrier(jnp.sum(rounded.astype(jnp.float32), axis=1))
        out_padded = jnp.concatenate([expert_out, jnp.zeros((1, D), jnp.float32)], axis=0)
        contribution = (weight_at[:, None] * out_padded[slot]).astype(jnp.bfloat16)
        return (total + contribution.astype(jnp.float32), None)
    total, _ = lax.scan(visit, jnp.zeros((BATCH_ROWS, D), jnp.float32), jnp.arange(EXPERTS, dtype=jnp.int32))
    return (wide + total).astype(jnp.bfloat16)
```

```python
import functools
import math

import jax
import jax.numpy as jnp
from jax import lax
from jax.experimental import pallas as pl
from jax.experimental.pallas import tpu as pltpu
from jax.sharding import PartitionSpec as P

D = 2880
QUERY_HEADS = 32
KEY_VALUE_HEADS = 4
HEAD_SIZE = 64
WINDOW_LENGTH = 128
TOP = 4


norm_eps = 1e-05
swish_alpha = 1.702
MIB = 1 << 20


def attend_kernel(
    len_ref, sink_ref, q_hbm, fk_hbm, fv_hbm, ck_hbm, cv_hbm, o_hbm, gu_hbm,
    out_ref, o_ref, gu_ref, q_ref, fk_ref, fv_ref, ck_ref, cv_ref, qs_ref, os_ref, sem
):
    ins = [(q_hbm, q_ref), (fk_hbm, fk_ref), (fv_hbm, fv_ref), (ck_hbm, ck_ref), (cv_hbm, cv_ref)]
    ahead = [(o_hbm, o_ref), (gu_hbm, gu_ref)]
    copies = [pltpu.make_async_copy(src, dst, sem.at[n]) for n, (src, dst) in enumerate(ins + ahead)]
    for copy in copies:
        copy.start()
    batch, width = q_ref.shape
    heads = sink_ref.shape[0]
    size = width // heads
    kv_heads = fk_ref.shape[1] // size
    group = heads // kv_heads
    window = ck_ref.shape[1]
    scale = 1.0 / math.sqrt(size)
    head_rows = lax.broadcasted_iota(jnp.int32, (heads, 1), 0)
    sink = jnp.zeros((heads, 1), jnp.float32)
    for h in range(heads):
        sink = jnp.where(head_rows == h, sink_ref[h], sink)
    qs_ref[...] = jnp.zeros(qs_ref.shape, jnp.float32)
    slots = lax.broadcasted_iota(jnp.int32, (heads, window), 1)
    copies[0].wait()
    q = q_ref[...].astype(jnp.float32)
    for h in range(heads):
        k = h // group
        qs_ref[:, h, k * size:(k + 1) * size] = q[:, h * size:(h + 1) * size]
    for copy in copies[1:len(ins)]:
        copy.wait()
    fk = fk_ref[...].astype(jnp.float32)
    fv = fv_ref[...].astype(jnp.float32)
    for b in range(batch):
        qb = qs_ref[b]
        scores = lax.dot_general(
            qb.astype(jnp.bfloat16), ck_ref[b], (((1,), (1,)), ((), ())), preferred_element_type=jnp.float32
        ) * scale
        own = jnp.sum(qb * fk[b:b + 1], axis=1, keepdims=True) * scale
        scores = jnp.where(slots >= window - len_ref[b], scores, -jnp.inf)
        top = jnp.maximum(jnp.maximum(jnp.max(scores, axis=1, keepdims=True), own), sink)
        probs = jnp.exp(scores - top)
        own = jnp.exp(own - top)
        total = jnp.sum(probs, axis=1, keepdims=True) + own + jnp.exp(sink - top)
        probs = (probs / total).astype(jnp.bfloat16)
        own = (own / total).astype(jnp.bfloat16).astype(jnp.float32)
        mixed = jnp.dot(probs, cv_ref[b], preferred_element_type=jnp.float32)
        os_ref[b] = mixed + own * fv[b:b + 1]
    for h in range(0, heads, 2):
        k0 = h // group
        k1 = (h + 1) // group
        pair = jnp.concatenate(
            [os_ref[:, h, k0 * size:(k0 + 1) * size], os_ref[:, h + 1, k1 * size:(k1 + 1) * size]], axis=1
        )
        out_ref[:, h * size:(h + 2) * size] = pair.astype(jnp.bfloat16)
    for copy in copies[len(ins):]:
        copy.wait()


VMEM = pl.BlockSpec(memory_space=pltpu.VMEM)
SMEM = pl.BlockSpec(memory_space=pltpu.SMEM)
HBM = pl.BlockSpec(memory_space=pltpu.HBM)


def attend_local(
    queries, fresh_key, fresh_value, cached_keys, cached_values, lengths, sink_logit_rows, o_weight, w_gate_up
):
    ins = [queries, fresh_key, fresh_value, cached_keys, cached_values]
    spread = (queries.shape[0], sink_logit_rows.shape[0], fresh_key.shape[1])
    return pl.pallas_call(
        attend_kernel,
        out_shape=[jax.ShapeDtypeStruct(a.shape, jnp.bfloat16) for a in (queries, o_weight, w_gate_up)],
        in_specs=[SMEM] * 2 + [HBM] * 7,
        out_specs=[VMEM] * 3,
        scratch_shapes=[pltpu.VMEM(a.shape, jnp.bfloat16) for a in ins] + [
            pltpu.VMEM(spread, jnp.float32),
            pltpu.VMEM(spread, jnp.float32),
            pltpu.SemaphoreType.DMA((len(ins) + 2,)),
        ],
        compiler_params=pltpu.CompilerParams(vmem_limit_bytes=32 * MIB),
        name="attend",
    )(lengths, sink_logit_rows, *[pltpu.with_memory_space_constraint(a, pltpu.HBM) for a in ins + [o_weight, w_gate_up]])


def project_kernel(*refs):
    blocks, (w_ref, res_ref, out_ref, rows_ref) = refs[:-4], refs[-4:]
    rows = blocks[0].shape[0]
    place = lax.axis_index("expert")
    for r, block in enumerate(blocks):
        rows_ref[pl.ds(pl.multiple_of((place ^ r) * rows, rows), rows), :] = block[...].astype(jnp.float32)
    projected = lax.dot_general(
        rows_ref[...].astype(jnp.bfloat16), w_ref[...], (((1,), (1,)), ((), ())), preferred_element_type=jnp.float32
    )
    out_ref[...] = (res_ref[...].astype(jnp.float32) + projected).astype(jnp.bfloat16)


def project(blocks, o_weight, residual):
    rows, width = blocks[0].shape
    return pl.pallas_call(
        project_kernel,
        out_shape=jax.ShapeDtypeStruct(residual.shape, jnp.bfloat16),
        in_specs=[VMEM] * (len(blocks) + 1) + [pl.BlockSpec(residual.shape, lambda: (0, 0))],
        out_specs=VMEM,
        scratch_shapes=[pltpu.VMEM((rows * len(blocks), width), jnp.float32)],
        compiler_params=pltpu.CompilerParams(vmem_limit_bytes=12 * MIB),
        name="project",
    )(*blocks, o_weight, residual)


def expert_kernel(*refs, lo, ys):
    halves = 2
    pairs = lo * ys
    near, far, keep, send = refs[:pairs], refs[pairs:2 * pairs], refs[2 * pairs + 5:3 * pairs + 5], refs[3 * pairs + 5:4 * pairs + 5]
    gain_ref, ids_ref, route_ref, gu_ref, down_ref = refs[2 * pairs:2 * pairs + 5]
    x_ref, weight_ref, down_buf, hidden_ref, sums_ref, sem = refs[4 * pairs + 5:]
    span, columns = near[0].shape
    width = x_ref.shape[1]
    units = down_buf.shape[0]
    members = ys * halves
    step = units // 3 if units % 48 == 0 else units
    group = lax.axis_index("dp")
    place = lax.axis_index("expert")
    copy = pltpu.make_async_copy(down_ref.at[0], down_buf, sem.at[0])
    copy.start()

    groups = weight_ref.shape[0]
    tokens = ids_ref.shape[1]
    rows = tokens // groups
    zs = span // rows
    weight = jnp.sum(jnp.where(ids_ref[...] == group, route_ref[...], 0.0), axis=0, keepdims=True)
    weight = jnp.transpose(jnp.broadcast_to(weight, (8, tokens)))[:, :1]
    for g in range(groups):
        weight_ref[g] = weight[g * rows:(g + 1) * rows]

    for x in range(lo):
        squares = jnp.zeros((span, 1), jnp.float32)
        for y in range(ys):
            for blocks in (near, far):
                v = blocks[x * ys + y][...].astype(jnp.float32)
                squares = squares + jnp.sum(v * v, axis=1, keepdims=True)
        scale = lax.rsqrt(squares / width + norm_eps)
        for p in range(members):
            @pl.when(place == p)
            def _():
                for r in range(members):
                    j = p ^ r
                    blocks = far if r % halves else near
                    gain = gain_ref[:, j * columns:(j + 1) * columns]
                    v = blocks[x * ys + r // halves][...].astype(jnp.float32)
                    x_ref[x * span:(x + 1) * span, j * columns:(j + 1) * columns] = (v * scale * gain).astype(jnp.bfloat16)

    x_all = x_ref[...]
    contract = (((1,), (1,)), ((), ()))
    for i in range(0, units, step):
        gate = lax.dot_general(x_all, gu_ref[0, 0, i:i + step, :], contract, preferred_element_type=jnp.float32)
        up = lax.dot_general(x_all, gu_ref[0, 1, i:i + step, :], contract, preferred_element_type=jnp.float32)
        hidden_ref[:, i:i + step] = ((up + 1.0) * gate * jax.nn.sigmoid(swish_alpha * gate)).astype(jnp.bfloat16)
    copy.wait()
    hidden = hidden_ref[...]
    for x in range(lo):
        part = jnp.dot(hidden[x * span:(x + 1) * span], down_buf[...], preferred_element_type=jnp.float32)
        scales = jnp.concatenate([weight_ref[group ^ (z * lo + x)] for z in range(zs)], axis=0)
        sums_ref[...] = (part * scales).astype(jnp.bfloat16)
        for p in range(members):
            @pl.when(place == p)
            def _():
                for r in range(members):
                    j = p ^ r
                    blocks = send if r % halves else keep
                    blocks[x * ys + r // halves][...] = sums_ref[:, j * columns:(j + 1) * columns]


def expert_sums(near, far, norm_gain, expert_ids, route_weights, w_gate_up, w_down, groups, lo):
    units, width = w_down.shape[1:]
    pairs = len(near)
    ys = pairs // lo
    span, columns = near[0].shape
    total = span * lo
    outs = pl.pallas_call(
        functools.partial(expert_kernel, lo=lo, ys=ys),
        out_shape=[jax.ShapeDtypeStruct((span, columns), jnp.bfloat16)] * (2 * pairs),
        in_specs=[VMEM] * (2 * pairs + 4) + [HBM],
        out_specs=[VMEM] * (2 * pairs),
        scratch_shapes=[
            pltpu.VMEM((total, width), jnp.bfloat16),
            pltpu.VMEM((groups, total // groups, 1), jnp.float32),
            pltpu.VMEM((units, width), jnp.bfloat16),
            pltpu.VMEM((total, units), jnp.bfloat16),
            pltpu.VMEM((span, width), jnp.bfloat16),
            pltpu.SemaphoreType.DMA((1,)),
        ],
        compiler_params=pltpu.CompilerParams(vmem_limit_bytes=36 * MIB),
        name="experts",
    )(
        *near, *far, norm_gain[None, :], expert_ids.T, route_weights.T, w_gate_up,
        pltpu.with_memory_space_constraint(w_down, pltpu.HBM)
    )
    return outs[:pairs], outs[pairs:]


def dense_body(
    queries, fresh_key, fresh_value, cached_keys, cached_values, lengths, sink_logit_rows, residual, o_weight,
    norm_gain, expert_ids, route_weights, w_gate_up, w_down
):
    groups = lax.axis_size("dp")
    members = lax.axis_size("expert")
    lo, halves = 2, 2
    zs, ys = groups // lo, members // halves
    rows = residual.shape[0]

    def swap(value, x=0, z=0, y=0, c=0):
        flip = (z * lo + x) * members + y * halves + c
        return lax.ppermute(value, ("dp", "expert"), [(i, i ^ flip) for i in range(groups * members)])

    attended, o_weight, w_gate_up = attend_local(
        queries, fresh_key, fresh_value, cached_keys, cached_values, lengths, sink_logit_rows, o_weight, w_gate_up
    )
    blocks = [attended] + [swap(attended, y=r // halves, c=r % halves) for r in range(1, members)]
    stream = project(blocks, o_weight, residual)

    others = [(x, y) for x in range(lo) for y in range(ys)][1:]
    line = jnp.concatenate([stream] + [swap(stream, z=z) for z in range(1, zs)], axis=0)
    near = [line] + [swap(line, x=x, y=y) for x, y in others]
    far = [swap(block, c=1) for block in near]
    keep, send = expert_sums(near, far, norm_gain, expert_ids, route_weights, w_gate_up, w_down, groups, lo)

    def added(parts):
        total = parts[0].astype(jnp.float32)
        for part in parts[1:]:
            total = total + part.astype(jnp.float32)
        return total

    def cut(value, i):
        return value[i * rows:(i + 1) * rows]

    chip = [added([own, swap(other, c=1)]).astype(jnp.bfloat16) for own, other in zip(keep, send)]
    plane = added([chip[0]] + [swap(part, x=x, y=y) for part, (x, y) in zip(chip[1:], others)]).astype(jnp.bfloat16)
    total = added([stream, cut(plane, 0)] + [swap(cut(plane, z), z=z) for z in range(1, zs)])
    return total.astype(jnp.bfloat16)


def attend(queries, fresh_key, fresh_value, cached_keys, cached_values, lengths, sink_logit_rows):
    batch_count = queries.shape[0]
    head_groups = QUERY_HEADS // KEY_VALUE_HEADS
    query_head_rows = queries.reshape(batch_count, KEY_VALUE_HEADS, head_groups, HEAD_SIZE)
    key_rows = cached_keys.reshape(batch_count, WINDOW_LENGTH, KEY_VALUE_HEADS, HEAD_SIZE)
    value_rows = cached_values.reshape(batch_count, WINDOW_LENGTH, KEY_VALUE_HEADS, HEAD_SIZE)
    score_scale = 1.0 / math.sqrt(HEAD_SIZE)
    cache_scores = (
        jnp.einsum("bkgd,bwkd->bkgw", query_head_rows, key_rows, preferred_element_type=jnp.float32)
        * score_scale
    )
    own_scores = (
        jnp.einsum(
            "npwm,npm->npw",
            query_head_rows,
            fresh_key.reshape(batch_count, KEY_VALUE_HEADS, HEAD_SIZE),
            preferred_element_type=jnp.float32,
        )
        * score_scale
    )
    slots = jnp.arange(WINDOW_LENGTH, dtype=jnp.int32)
    valid = (slots[None, :] >= (WINDOW_LENGTH - lengths)[:, None])[:, None, None, :]
    sink_terms = sink_logit_rows.reshape(KEY_VALUE_HEADS, head_groups)[None]
    masked = jnp.where(valid, cache_scores, -jnp.inf)
    top = jnp.maximum(jnp.maximum(jnp.max(masked, axis=-1), own_scores), sink_terms)
    cache_exp = jnp.where(valid, jnp.exp(masked - top[..., None]), 0.0)
    self_exp = jnp.exp(own_scores - top)
    total = jnp.sum(cache_exp, axis=-1) + self_exp + jnp.exp(sink_terms - top)
    cache_prob = (cache_exp / total[..., None]).astype(jnp.bfloat16)
    own_probability = (self_exp / total).astype(jnp.bfloat16)
    blended = jnp.einsum(
        "bkgw,bwkd->bkgd", cache_prob, value_rows, preferred_element_type=jnp.float32
    )
    blended = blended + own_probability.astype(jnp.float32)[..., None] * fresh_value.reshape(
        batch_count, KEY_VALUE_HEADS, 1, HEAD_SIZE
    ).astype(jnp.float32)
    return blended.reshape(batch_count, QUERY_HEADS * HEAD_SIZE).astype(jnp.bfloat16)


def slot_onehot(named, capacity):
    counts = jnp.cumsum(named.astype(jnp.int32), axis=1) - 1
    places = jnp.arange(capacity, dtype=jnp.int32)
    return named[:, None, :] & (counts[:, None, :] == places[None, :, None])


def receiver_slots(expert_ids, route_weights, expert, blocks, capacity):
    picked = expert_ids == expert
    named = jnp.any(picked, axis=1).reshape(blocks, -1)
    weight_at = jnp.sum(jnp.where(picked, route_weights, 0.0), axis=1).reshape(blocks, -1)
    onehot = slot_onehot(named, capacity)
    slot_weight = jnp.sum(jnp.where(onehot, weight_at[:, None, :], 0.0), axis=2)
    return (onehot, slot_weight)


def sender_slots(my_ids, experts, capacity):
    labels = jnp.arange(experts, dtype=jnp.int32)
    named = jnp.any(my_ids[None, :, :] == labels[:, None, None], axis=2)
    return slot_onehot(named, capacity)


def body(
    queries,
    fresh_key,
    fresh_value,
    cached_keys,
    cached_values,
    lengths,
    sink_logit_rows,
    residual,
    o_weight,
    norm_gain,
    expert_ids,
    route_weights,
    w_gate_up,
    w_down,
):
    attended = attend(
        queries, fresh_key, fresh_value, cached_keys, cached_values, lengths, sink_logit_rows
    )
    projected = lax.dot_general(
        lax.all_gather(attended, "expert", axis=0, tiled=True),
        o_weight,
        (((1,), (1,)), ((), ())),
        preferred_element_type=jnp.float32,
    )
    stream = (residual.astype(jnp.float32) + projected).astype(jnp.bfloat16)
    wide = stream.astype(jnp.float32)
    group_rows = stream.shape[0]
    columns = stream.shape[1]
    experts = lax.axis_size("dp")
    capacity = 2 * group_rows * TOP // experts
    gain_cols = lax.dynamic_slice_in_dim(norm_gain, lax.axis_index("expert") * columns, columns)
    squares = lax.psum(jnp.sum(wide * wide, axis=1), "expert")
    score_scale = lax.rsqrt(squares / D + norm_eps)
    outgoing = (wide * score_scale[:, None] * gain_cols[None, :]).astype(jnp.bfloat16)
    onehot_in, slot_weight = receiver_slots(
        expert_ids, route_weights, lax.axis_index("dp"), experts, capacity
    )
    my_ids = lax.dynamic_slice_in_dim(expert_ids, lax.axis_index("dp") * group_rows, group_rows, 0)
    onehot_out = sender_slots(my_ids, experts, capacity)
    outbound = jnp.einsum(
        "ect,td->ecd", onehot_out.astype(jnp.bfloat16), outgoing, preferred_element_type=jnp.float32
    ).astype(jnp.bfloat16)
    received = lax.all_to_all(outbound, "dp", split_axis=0, concat_axis=0, tiled=True)
    rows = received.reshape(experts * capacity, columns)
    gate_up = w_gate_up[0]
    down = w_down[0]
    both = jnp.einsum(
        "rc,hfc->rhf",
        lax.all_gather(rows, "expert", axis=1, tiled=True),
        gate_up,
        preferred_element_type=jnp.float32,
    )
    gate = both[:, 0]
    up = both[:, 1]
    hidden = ((up + 1.0) * gate * jax.nn.sigmoid(swish_alpha * gate)).astype(jnp.bfloat16)
    summed = lax.psum_scatter(
        lax.dot_general(
            down, hidden, (((0,), (1,)), ((), ())), preferred_element_type=jnp.float32
        ).astype(jnp.bfloat16),
        "expert",
        scatter_dimension=0,
        tiled=True,
    ).astype(jnp.float32)
    contribution = (summed * slot_weight.reshape(1, -1)).astype(jnp.bfloat16)
    contribution = contribution.T.reshape(experts, capacity, columns)
    returned = lax.all_to_all(contribution, "dp", split_axis=0, concat_axis=0, tiled=True)
    returned_sum = jnp.einsum(
        "ect,ecd->td",
        onehot_out.astype(jnp.float32),
        returned.astype(jnp.float32),
        precision=lax.Precision.HIGHEST,
    )
    return (wide + returned_sum).astype(jnp.bfloat16)


def solution(mesh):
    placed = (
        P(("dp", "expert"), None),
        P(("dp", "expert"), None),
        P(("dp", "expert"), None),
        P(("dp", "expert"), None, None),
        P(("dp", "expert"), None, None),
        P(("dp", "expert")),
        P(),
        P("dp", "expert"),
        P("expert", None),
        P(),
        P(),
        P(),
        P("dp", None, "expert", None),
        P("dp", "expert", None),
    )

    def layer(*args):
        group_rows = args[7].shape[0]
        groups, members = mesh.shape["dp"], mesh.shape["expert"]
        capacity = 2 * group_rows * TOP // groups
        paired = groups & (groups - 1) == 0 and members & (members - 1) == 0 and groups > 1 and members > 1
        return (dense_body if capacity >= group_rows and paired else body)(*args)

    return jax.shard_map(
        layer, mesh=mesh, in_specs=placed, out_specs=P("dp", "expert"), check_vma=False
    )
```

```python
import functools
import math

import jax
import jax.numpy as jnp
from jax import lax
from jax.experimental import pallas as pl
from jax.experimental.pallas import tpu as pltpu
from jax.sharding import PartitionSpec as P

D = 2880
QUERY_HEADS = 32
KEY_VALUE_HEADS = 4
HEAD_SIZE = 64
WINDOW_LENGTH = 128
TOP = 4


norm_eps = 1e-05
swish_alpha = 1.702
MIB = 1 << 20


def attend_kernel(
    len_hbm, sink_hbm, q_hbm, fk_hbm, fv_hbm, ck_hbm, cv_hbm, o_hbm, gu_hbm,
    out_ref, o_ref, gu_ref, len_ref, sink_ref, q_ref, fk_ref, fv_ref, ck_ref, cv_ref, qs_ref, os_ref, sem
):
    ins = [
        (q_hbm, q_ref), (len_hbm, len_ref), (sink_hbm, sink_ref), (fk_hbm, fk_ref), (fv_hbm, fv_ref),
        (ck_hbm, ck_ref), (cv_hbm, cv_ref)
    ]
    ahead = [(o_hbm, o_ref), (gu_hbm.at[:, 0], gu_ref)]
    copies = [pltpu.make_async_copy(src, dst, sem.at[n]) for n, (src, dst) in enumerate(ins + ahead)]
    for copy in copies:
        copy.start()
    batch, width = q_ref.shape
    heads = sink_ref.shape[0]
    size = width // heads
    kv_heads = fk_ref.shape[1] // size
    group = heads // kv_heads
    window = ck_ref.shape[1]
    scale = 1.0 / math.sqrt(size)
    qs_ref[...] = jnp.zeros(qs_ref.shape, jnp.float32)
    slots = lax.broadcasted_iota(jnp.int32, (heads, window), 1)
    head_rows = lax.broadcasted_iota(jnp.int32, (heads, 1), 0)
    copies[0].wait()
    q = q_ref[...].astype(jnp.float32)
    for h in range(heads):
        k = h // group
        qs_ref[:, h, k * size:(k + 1) * size] = q[:, h * size:(h + 1) * size]
    for copy in copies[1:5]:
        copy.wait()
    sink = jnp.zeros((heads, 1), jnp.float32)
    for h in range(heads):
        sink = jnp.where(head_rows == h, sink_ref[h], sink)
    fk = fk_ref[...].astype(jnp.float32)
    fv = fv_ref[...].astype(jnp.float32)
    copies[5].wait()
    scores, owns = [], []
    for b in range(batch):
        qb = qs_ref[b]
        score = lax.dot_general(
            qb.astype(jnp.bfloat16), ck_ref[b], (((1,), (1,)), ((), ())), preferred_element_type=jnp.float32
        ) * scale
        scores.append(jnp.where(slots >= window - len_ref[b], score, -jnp.inf))
        owns.append(jnp.sum(qb * fk[b:b + 1], axis=1, keepdims=True) * scale)
    scores = jnp.concatenate(scores, axis=0)
    own = jnp.concatenate(owns, axis=0)
    sink = jnp.concatenate([sink] * batch, axis=0)
    top = jnp.maximum(jnp.maximum(jnp.max(scores, axis=1, keepdims=True), own), sink)
    probs = jnp.exp(scores - top)
    own = jnp.exp(own - top)
    total = jnp.sum(probs, axis=1, keepdims=True) + own + jnp.exp(sink - top)
    share = 1.0 / total
    probs = (probs * share).astype(jnp.bfloat16)
    own = (own * share).astype(jnp.bfloat16).astype(jnp.float32)
    copies[6].wait()
    for b in range(batch):
        part = slice(b * heads, (b + 1) * heads)
        os_ref[b] = jnp.dot(probs[part], cv_ref[b], preferred_element_type=jnp.float32) + own[part] * fv[b:b + 1]
    for h in range(0, heads, 2):
        k0 = h // group
        k1 = (h + 1) // group
        pair = jnp.concatenate(
            [os_ref[:, h, k0 * size:(k0 + 1) * size], os_ref[:, h + 1, k1 * size:(k1 + 1) * size]], axis=1
        )
        out_ref[:, h * size:(h + 2) * size] = pair.astype(jnp.bfloat16)
    for copy in copies[len(ins):]:
        copy.wait()


VMEM = pl.BlockSpec(memory_space=pltpu.VMEM)
SMEM = pl.BlockSpec(memory_space=pltpu.SMEM)
HBM = pl.BlockSpec(memory_space=pltpu.HBM)


def in_hbm(array):
    return pltpu.with_memory_space_constraint(array, pltpu.HBM)


def attend_local(
    queries, fresh_key, fresh_value, cached_keys, cached_values, lengths, sink_logit_rows, o_weight, w_gate_up
):
    arrays = [queries, fresh_key, fresh_value, cached_keys, cached_values]
    small = [lengths, sink_logit_rows]
    spread = (queries.shape[0], sink_logit_rows.shape[0], fresh_key.shape[1])
    gate_shape = w_gate_up.shape[:1] + w_gate_up.shape[2:]
    return pl.pallas_call(
        attend_kernel,
        out_shape=[jax.ShapeDtypeStruct(shape, jnp.bfloat16) for shape in (queries.shape, o_weight.shape, gate_shape)],
        in_specs=[HBM] * 9,
        out_specs=[VMEM] * 3,
        scratch_shapes=[pltpu.SMEM(a.shape, a.dtype) for a in small] + [
            pltpu.VMEM(a.shape, a.dtype) for a in arrays
        ] + [
            pltpu.VMEM(spread, jnp.float32),
            pltpu.VMEM(spread, jnp.float32),
            pltpu.SemaphoreType.DMA((9,)),
        ],
        compiler_params=pltpu.CompilerParams(vmem_limit_bytes=32 * MIB),
        name="attend",
    )(*[in_hbm(a) for a in small + arrays + [o_weight, w_gate_up]])


def project_kernel(*refs):
    blocks, (w_ref, res_ref, out_ref, rows_ref) = refs[:-4], refs[-4:]
    rows = blocks[0].shape[0]
    place = lax.axis_index("expert")
    for r, block in enumerate(blocks):
        rows_ref[pl.ds(pl.multiple_of((place ^ r) * rows, rows), rows), :] = block[...].astype(jnp.float32)
    projected = lax.dot_general(
        rows_ref[...].astype(jnp.bfloat16), w_ref[...], (((1,), (1,)), ((), ())), preferred_element_type=jnp.float32
    )
    out_ref[...] = (res_ref[...].astype(jnp.float32) + projected).astype(jnp.bfloat16)


def project(blocks, o_weight, residual):
    rows, width = blocks[0].shape
    return pl.pallas_call(
        project_kernel,
        out_shape=jax.ShapeDtypeStruct(residual.shape, jnp.bfloat16),
        in_specs=[VMEM] * (len(blocks) + 1) + [pl.BlockSpec(residual.shape, lambda: (0, 0))],
        out_specs=VMEM,
        scratch_shapes=[pltpu.VMEM((rows * len(blocks), width), jnp.float32)],
        compiler_params=pltpu.CompilerParams(vmem_limit_bytes=12 * MIB),
        name="project",
    )(*blocks, o_weight, residual)


def expert_kernel(*refs, lo, ys):
    halves = 2
    pairs = lo * ys
    near, far, (gain_ref, ids_ref, route_ref, gate_ref, gu_hbm, down_hbm) = (
        refs[:pairs], refs[pairs:2 * pairs], refs[2 * pairs:2 * pairs + 6]
    )
    refs = refs[2 * pairs + 6:]
    keep, send = refs[:pairs], refs[pairs:2 * pairs]
    x_ref, weight_ref, up_ref, down_ref, hidden_ref, sums_ref, sem = refs[2 * pairs:]
    span, columns = near[0].shape
    width = x_ref.shape[1]
    members = ys * halves
    group = lax.axis_index("dp")
    place = lax.axis_index("expert")
    up_copy = pltpu.make_async_copy(gu_hbm.at[0, 1], up_ref, sem.at[0])
    down_copy = pltpu.make_async_copy(down_hbm.at[0], down_ref, sem.at[1])
    up_copy.start()
    down_copy.start()

    groups = weight_ref.shape[0]
    tokens = ids_ref.shape[1]
    rows = tokens // groups
    zs = span // rows
    weight = jnp.sum(jnp.where(ids_ref[...] == group, route_ref[...], 0.0), axis=0, keepdims=True)
    weight = jnp.transpose(jnp.broadcast_to(weight, (8, tokens)))[:, :1]
    for g in range(groups):
        weight_ref[g] = weight[g * rows:(g + 1) * rows]

    scales = []
    for x in range(lo):
        squares = jnp.zeros((span, columns), jnp.float32)
        for y in range(ys):
            for blocks in (near, far):
                v = blocks[x * ys + y][...].astype(jnp.float32)
                squares = squares + v * v
        scales.append(lax.rsqrt(jnp.sum(squares, axis=1, keepdims=True) / width + norm_eps))
    for p in range(members):
        @pl.when(place == p)
        def _():
            for x in range(lo):
                for r in range(members):
                    j = p ^ r
                    blocks = far if r % halves else near
                    gain = gain_ref[:, j * columns:(j + 1) * columns]
                    v = blocks[x * ys + r // halves][...].astype(jnp.float32)
                    x_ref[x * span:(x + 1) * span, j * columns:(j + 1) * columns] = (
                        v * scales[x] * gain
                    ).astype(jnp.bfloat16)

    x_all = x_ref[...]
    contract = (((1,), (1,)), ((), ()))
    gate = lax.dot_general(x_all, gate_ref[0], contract, preferred_element_type=jnp.float32)
    gate = gate * jax.nn.sigmoid(swish_alpha * gate)
    up_copy.wait()
    up = lax.dot_general(x_all, up_ref[...], contract, preferred_element_type=jnp.float32)
    hidden_ref[...] = ((up + 1.0) * gate).astype(jnp.bfloat16)
    down_copy.wait()
    scale = jnp.concatenate([weight_ref[group ^ (z * lo + x)] for x in range(lo) for z in range(zs)], axis=0)
    hidden = hidden_ref[...]
    for i in range(0, width, 768):
        part = slice(i, min(i + 768, width))
        sums_ref[:, part] = (
            jnp.dot(hidden, down_ref[:, part], preferred_element_type=jnp.float32) * scale
        ).astype(jnp.bfloat16)
    for p in range(members):
        @pl.when(place == p)
        def _():
            for x in range(lo):
                for r in range(members):
                    j = p ^ r
                    blocks = send if r % halves else keep
                    blocks[x * ys + r // halves][...] = sums_ref[
                        x * span:(x + 1) * span, j * columns:(j + 1) * columns
                    ]


def expert_sums(near, far, norm_gain, expert_ids, route_weights, w_gate, w_gate_up, w_down, groups, lo):
    units, width = w_down.shape[1:]
    pairs = len(near)
    ys = pairs // lo
    span, columns = near[0].shape
    total = span * lo
    outs = pl.pallas_call(
        functools.partial(expert_kernel, lo=lo, ys=ys),
        out_shape=[jax.ShapeDtypeStruct((span, columns), jnp.bfloat16)] * (2 * pairs),
        in_specs=[VMEM] * (2 * pairs + 4) + [HBM] * 2,
        out_specs=[VMEM] * (2 * pairs),
        scratch_shapes=[
            pltpu.VMEM((total, width), jnp.bfloat16),
            pltpu.VMEM((groups, total // groups, 1), jnp.float32),
            pltpu.VMEM((units, width), jnp.bfloat16),
            pltpu.VMEM((units, width), jnp.bfloat16),
            pltpu.VMEM((total, units), jnp.bfloat16),
            pltpu.VMEM((total, width), jnp.bfloat16),
            pltpu.SemaphoreType.DMA((2,)),
        ],
        compiler_params=pltpu.CompilerParams(vmem_limit_bytes=36 * MIB),
        name="experts",
    )(
        *near, *far, norm_gain[None, :], expert_ids.T, route_weights.T, w_gate, in_hbm(w_gate_up), in_hbm(w_down)
    )
    return outs[:pairs], outs[pairs:]


def dense_body(
    queries, fresh_key, fresh_value, cached_keys, cached_values, lengths, sink_logit_rows, residual, o_weight,
    norm_gain, expert_ids, route_weights, w_gate_up, w_down
):
    groups = lax.axis_size("dp")
    members = lax.axis_size("expert")
    lo, halves = 2, 2
    zs, ys = groups // lo, members // halves
    rows = residual.shape[0]

    def swap(value, x=0, z=0, y=0, c=0):
        flip = (z * lo + x) * members + y * halves + c
        return lax.ppermute(value, ("dp", "expert"), [(i, i ^ flip) for i in range(groups * members)])

    attended, o_weight, w_gate = attend_local(
        queries, fresh_key, fresh_value, cached_keys, cached_values, lengths, sink_logit_rows, o_weight, w_gate_up
    )
    blocks = [attended] + [swap(attended, y=r // halves, c=r % halves) for r in range(1, members)]
    stream = project(blocks, o_weight, residual)

    others = [(x, y) for x in range(lo) for y in range(ys)][1:]
    line = jnp.concatenate([stream] + [swap(stream, z=z) for z in range(1, zs)], axis=0)
    near = [line] + [swap(line, x=x, y=y) for x, y in others]
    far = [swap(block, c=1) for block in near]
    keep, send = expert_sums(near, far, norm_gain, expert_ids, route_weights, w_gate, w_gate_up, w_down, groups, lo)

    def added(parts):
        total = parts[0].astype(jnp.float32)
        for part in parts[1:]:
            total = total + part.astype(jnp.float32)
        return total

    def cut(value, i):
        return value[i * rows:(i + 1) * rows]

    chip = [added([own, swap(other, c=1)]).astype(jnp.bfloat16) for own, other in zip(keep, send)]
    corner = added([cut(chip[3], 0)] + [swap(cut(chip[3], z), z=z) for z in range(1, zs)]).astype(jnp.bfloat16)
    plane = added([chip[0], swap(chip[1], y=1), swap(chip[2], x=1)]).astype(jnp.bfloat16)
    total = added([stream, cut(plane, 0)] + [swap(cut(plane, z), z=z) for z in range(1, zs)] + [swap(corner, x=1, y=1)])
    return total.astype(jnp.bfloat16)


def attend(queries, fresh_key, fresh_value, cached_keys, cached_values, lengths, sink_logit_rows):
    batch_count = queries.shape[0]
    head_groups = QUERY_HEADS // KEY_VALUE_HEADS
    query_head_rows = queries.reshape(batch_count, KEY_VALUE_HEADS, head_groups, HEAD_SIZE)
    key_rows = cached_keys.reshape(batch_count, WINDOW_LENGTH, KEY_VALUE_HEADS, HEAD_SIZE)
    value_rows = cached_values.reshape(batch_count, WINDOW_LENGTH, KEY_VALUE_HEADS, HEAD_SIZE)
    score_scale = 1.0 / math.sqrt(HEAD_SIZE)
    cache_scores = (
        jnp.einsum("bkgd,bwkd->bkgw", query_head_rows, key_rows, preferred_element_type=jnp.float32)
        * score_scale
    )
    own_scores = (
        jnp.einsum(
            "npwm,npm->npw",
            query_head_rows,
            fresh_key.reshape(batch_count, KEY_VALUE_HEADS, HEAD_SIZE),
            preferred_element_type=jnp.float32,
        )
        * score_scale
    )
    slots = jnp.arange(WINDOW_LENGTH, dtype=jnp.int32)
    valid = (slots[None, :] >= (WINDOW_LENGTH - lengths)[:, None])[:, None, None, :]
    sink_terms = sink_logit_rows.reshape(KEY_VALUE_HEADS, head_groups)[None]
    masked = jnp.where(valid, cache_scores, -jnp.inf)
    top = jnp.maximum(jnp.maximum(jnp.max(masked, axis=-1), own_scores), sink_terms)
    cache_exp = jnp.where(valid, jnp.exp(masked - top[..., None]), 0.0)
    self_exp = jnp.exp(own_scores - top)
    total = jnp.sum(cache_exp, axis=-1) + self_exp + jnp.exp(sink_terms - top)
    cache_prob = (cache_exp / total[..., None]).astype(jnp.bfloat16)
    own_probability = (self_exp / total).astype(jnp.bfloat16)
    blended = jnp.einsum(
        "bkgw,bwkd->bkgd", cache_prob, value_rows, preferred_element_type=jnp.float32
    )
    blended = blended + own_probability.astype(jnp.float32)[..., None] * fresh_value.reshape(
        batch_count, KEY_VALUE_HEADS, 1, HEAD_SIZE
    ).astype(jnp.float32)
    return blended.reshape(batch_count, QUERY_HEADS * HEAD_SIZE).astype(jnp.bfloat16)


def slot_onehot(named, capacity):
    counts = jnp.cumsum(named.astype(jnp.int32), axis=1) - 1
    places = jnp.arange(capacity, dtype=jnp.int32)
    return named[:, None, :] & (counts[:, None, :] == places[None, :, None])


def receiver_slots(expert_ids, route_weights, expert, blocks, capacity):
    picked = expert_ids == expert
    named = jnp.any(picked, axis=1).reshape(blocks, -1)
    weight_at = jnp.sum(jnp.where(picked, route_weights, 0.0), axis=1).reshape(blocks, -1)
    onehot = slot_onehot(named, capacity)
    slot_weight = jnp.sum(jnp.where(onehot, weight_at[:, None, :], 0.0), axis=2)
    return (onehot, slot_weight)


def sender_slots(my_ids, experts, capacity):
    labels = jnp.arange(experts, dtype=jnp.int32)
    named = jnp.any(my_ids[None, :, :] == labels[:, None, None], axis=2)
    return slot_onehot(named, capacity)


def body(
    queries,
    fresh_key,
    fresh_value,
    cached_keys,
    cached_values,
    lengths,
    sink_logit_rows,
    residual,
    o_weight,
    norm_gain,
    expert_ids,
    route_weights,
    w_gate_up,
    w_down,
):
    attended = attend(
        queries, fresh_key, fresh_value, cached_keys, cached_values, lengths, sink_logit_rows
    )
    projected = lax.dot_general(
        lax.all_gather(attended, "expert", axis=0, tiled=True),
        o_weight,
        (((1,), (1,)), ((), ())),
        preferred_element_type=jnp.float32,
    )
    stream = (residual.astype(jnp.float32) + projected).astype(jnp.bfloat16)
    wide = stream.astype(jnp.float32)
    group_rows = stream.shape[0]
    columns = stream.shape[1]
    experts = lax.axis_size("dp")
    capacity = 2 * group_rows * TOP // experts
    gain_cols = lax.dynamic_slice_in_dim(norm_gain, lax.axis_index("expert") * columns, columns)
    squares = lax.psum(jnp.sum(wide * wide, axis=1), "expert")
    score_scale = lax.rsqrt(squares / D + norm_eps)
    outgoing = (wide * score_scale[:, None] * gain_cols[None, :]).astype(jnp.bfloat16)
    onehot_in, slot_weight = receiver_slots(
        expert_ids, route_weights, lax.axis_index("dp"), experts, capacity
    )
    my_ids = lax.dynamic_slice_in_dim(expert_ids, lax.axis_index("dp") * group_rows, group_rows, 0)
    onehot_out = sender_slots(my_ids, experts, capacity)
    outbound = jnp.einsum(
        "ect,td->ecd", onehot_out.astype(jnp.bfloat16), outgoing, preferred_element_type=jnp.float32
    ).astype(jnp.bfloat16)
    received = lax.all_to_all(outbound, "dp", split_axis=0, concat_axis=0, tiled=True)
    rows = received.reshape(experts * capacity, columns)
    gate_up = w_gate_up[0]
    down = w_down[0]
    both = jnp.einsum(
        "rc,hfc->rhf",
        lax.all_gather(rows, "expert", axis=1, tiled=True),
        gate_up,
        preferred_element_type=jnp.float32,
    )
    gate = both[:, 0]
    up = both[:, 1]
    hidden = ((up + 1.0) * gate * jax.nn.sigmoid(swish_alpha * gate)).astype(jnp.bfloat16)
    summed = lax.psum_scatter(
        lax.dot_general(
            down, hidden, (((0,), (1,)), ((), ())), preferred_element_type=jnp.float32
        ).astype(jnp.bfloat16),
        "expert",
        scatter_dimension=0,
        tiled=True,
    ).astype(jnp.float32)
    contribution = (summed * slot_weight.reshape(1, -1)).astype(jnp.bfloat16)
    contribution = contribution.T.reshape(experts, capacity, columns)
    returned = lax.all_to_all(contribution, "dp", split_axis=0, concat_axis=0, tiled=True)
    returned_sum = jnp.einsum(
        "ect,ecd->td",
        onehot_out.astype(jnp.float32),
        returned.astype(jnp.float32),
        precision=lax.Precision.HIGHEST,
    )
    return (wide + returned_sum).astype(jnp.bfloat16)


def solution(mesh):
    placed = (
        P(("dp", "expert"), None),
        P(("dp", "expert"), None),
        P(("dp", "expert"), None),
        P(("dp", "expert"), None, None),
        P(("dp", "expert"), None, None),
        P(("dp", "expert")),
        P(),
        P("dp", "expert"),
        P("expert", None),
        P(),
        P(),
        P(),
        P("dp", None, "expert", None),
        P("dp", "expert", None),
    )

    def layer(*args):
        group_rows = args[7].shape[0]
        groups, members = mesh.shape["dp"], mesh.shape["expert"]
        capacity = 2 * group_rows * TOP // groups
        paired = groups & (groups - 1) == 0 and groups > 1 and members == 4
        return (dense_body if capacity >= group_rows and paired else body)(*args)

    return jax.shard_map(
        layer, mesh=mesh, in_specs=placed, out_specs=P("dp", "expert"), check_vma=False
    )
```

```python
import functools
import math

import jax
import jax.numpy as jnp
from jax import lax
from jax.experimental import pallas as pl
from jax.experimental.pallas import tpu as pltpu
from jax.sharding import PartitionSpec as P


D = 2880
QUERY_HEADS = 32
KEY_VALUE_HEADS = 4
HEAD_SIZE = 64
WINDOW_LENGTH = 128
TOP = 4


norm_eps = 1e-05
swish_alpha = 1.702
MIB = 1 << 20


def attend_kernel(
    len_hbm, sink_hbm, q_hbm, fk_hbm, fv_hbm, ck_hbm, cv_hbm, gu_hbm,
    out_ref, gu_ref, len_ref, sink_ref, q_ref, fk_ref, fv_ref, ck_ref, cv_ref, qs_ref, os_ref, sem
):
    ins = [
        (q_hbm, q_ref), (len_hbm, len_ref), (sink_hbm, sink_ref), (fk_hbm, fk_ref), (fv_hbm, fv_ref),
        (ck_hbm, ck_ref), (cv_hbm, cv_ref)
    ]
    ahead = [(gu_hbm.at[:, 0], gu_ref)]
    copies = [pltpu.make_async_copy(src, dst, sem.at[n]) for n, (src, dst) in enumerate(ins + ahead)]
    for copy in copies:
        copy.start()
    batch, width = q_ref.shape
    heads = sink_ref.shape[0]
    size = width // heads
    kv_heads = fk_ref.shape[1] // size
    group = heads // kv_heads
    window = ck_ref.shape[1]
    scale = 1.0 / math.sqrt(size)
    qs_ref[...] = jnp.zeros(qs_ref.shape, jnp.float32)
    slots = lax.broadcasted_iota(jnp.int32, (heads, window), 1)
    head_rows = lax.broadcasted_iota(jnp.int32, (heads, 1), 0)
    copies[0].wait()
    q = q_ref[...].astype(jnp.float32)
    for h in range(heads):
        k = h // group
        qs_ref[:, h, k * size:(k + 1) * size] = q[:, h * size:(h + 1) * size]
    for copy in copies[1:5]:
        copy.wait()
    sink = jnp.zeros((heads, 1), jnp.float32)
    for h in range(heads):
        sink = jnp.where(head_rows == h, sink_ref[h], sink)
    fk = fk_ref[...].astype(jnp.float32)
    fv = fv_ref[...].astype(jnp.float32)
    copies[5].wait()
    scores, owns = [], []
    for b in range(batch):
        qb = qs_ref[b]
        score = lax.dot_general(
            qb.astype(jnp.bfloat16), ck_ref[b], (((1,), (1,)), ((), ())), preferred_element_type=jnp.float32
        ) * scale
        scores.append(jnp.where(slots >= window - len_ref[b], score, -jnp.inf))
        owns.append(jnp.sum(qb * fk[b:b + 1], axis=1, keepdims=True) * scale)
    scores = jnp.concatenate(scores, axis=0)
    own = jnp.concatenate(owns, axis=0)
    sink = jnp.concatenate([sink] * batch, axis=0)
    top = jnp.maximum(jnp.maximum(jnp.max(scores, axis=1, keepdims=True), own), sink)
    probs = jnp.exp(scores - top)
    own = jnp.exp(own - top)
    total = jnp.sum(probs, axis=1, keepdims=True) + own + jnp.exp(sink - top)
    share = 1.0 / total
    probs = (probs * share).astype(jnp.bfloat16)
    own = (own * share).astype(jnp.bfloat16).astype(jnp.float32)
    copies[6].wait()
    for b in range(batch):
        part = slice(b * heads, (b + 1) * heads)
        os_ref[b] = jnp.dot(probs[part], cv_ref[b], preferred_element_type=jnp.float32) + own[part] * fv[b:b + 1]
    for h in range(0, heads, 2):
        k0 = h // group
        k1 = (h + 1) // group
        pair = jnp.concatenate(
            [os_ref[:, h, k0 * size:(k0 + 1) * size], os_ref[:, h + 1, k1 * size:(k1 + 1) * size]], axis=1
        )
        out_ref[:, h * size:(h + 2) * size] = pair.astype(jnp.bfloat16)
    for copy in copies[len(ins):]:
        copy.wait()


VMEM = pl.BlockSpec(memory_space=pltpu.VMEM)
SMEM = pl.BlockSpec(memory_space=pltpu.SMEM)
HBM = pl.BlockSpec(memory_space=pltpu.HBM)


def in_hbm(array):
    return pltpu.with_memory_space_constraint(array, pltpu.HBM)


def attend_local(
    queries, fresh_key, fresh_value, cached_keys, cached_values, lengths, sink_logit_rows, w_gate_up
):
    arrays = [queries, fresh_key, fresh_value, cached_keys, cached_values]
    small = [lengths, sink_logit_rows]
    spread = (queries.shape[0], sink_logit_rows.shape[0], fresh_key.shape[1])
    gate_shape = w_gate_up.shape[:1] + w_gate_up.shape[2:]
    return pl.pallas_call(
        attend_kernel,
        out_shape=[jax.ShapeDtypeStruct(shape, jnp.bfloat16) for shape in (queries.shape, gate_shape)],
        in_specs=[HBM] * 8,
        out_specs=[VMEM] * 2,
        scratch_shapes=[pltpu.SMEM(a.shape, a.dtype) for a in small] + [
            pltpu.VMEM(a.shape, a.dtype) for a in arrays
        ] + [
            pltpu.VMEM(spread, jnp.float32),
            pltpu.VMEM(spread, jnp.float32),
            pltpu.SemaphoreType.DMA((8,)),
        ],
        compiler_params=pltpu.CompilerParams(vmem_limit_bytes=32 * MIB),
        name="attend",
    )(*[in_hbm(a) for a in small + arrays + [w_gate_up]])


def bring_kernel(after_ref, source_hbm, target_ref, sem):
    copy = pltpu.make_async_copy(source_hbm, target_ref, sem.at[0])
    copy.start()
    copy.wait()


def bring(after, weight):
    call = pl.pallas_call(
        bring_kernel,
        out_shape=jax.ShapeDtypeStruct(weight.shape, weight.dtype),
        in_specs=[VMEM, HBM],
        out_specs=VMEM,
        scratch_shapes=[pltpu.SemaphoreType.DMA((1,))],
        compiler_params=pltpu.CompilerParams(vmem_limit_bytes=8 * MIB),
        cost_estimate=pl.CostEstimate(flops=10**9, bytes_accessed=4 * MIB, transcendentals=0),
        name="bring",
    )
    weight = in_hbm(weight)
    return call(after, weight)


def project_kernel(*refs):
    blocks, (w_ref, res_ref, out_ref, rows_ref) = refs[:-4], refs[-4:]
    rows = blocks[0].shape[0]
    place = lax.axis_index("expert")
    for r, block in enumerate(blocks):
        rows_ref[pl.ds(pl.multiple_of((place ^ r) * rows, rows), rows), :] = block[...].astype(jnp.float32)
    projected = lax.dot_general(
        rows_ref[...].astype(jnp.bfloat16), w_ref[...], (((1,), (1,)), ((), ())), preferred_element_type=jnp.float32
    )
    out_ref[...] = (res_ref[...].astype(jnp.float32) + projected).astype(jnp.bfloat16)


def project(blocks, o_weight, residual):
    rows, width = blocks[0].shape
    return pl.pallas_call(
        project_kernel,
        out_shape=jax.ShapeDtypeStruct(residual.shape, jnp.bfloat16),
        in_specs=[VMEM] * (len(blocks) + 1) + [pl.BlockSpec(residual.shape, lambda: (0, 0))],
        out_specs=VMEM,
        scratch_shapes=[pltpu.VMEM((rows * len(blocks), width), jnp.float32)],
        compiler_params=pltpu.CompilerParams(vmem_limit_bytes=12 * MIB),
        name="project",
    )(*blocks, o_weight, residual)


def expert_kernel(*refs, lo, ys):
    halves = 2
    pairs = lo * ys
    near, far, (gain_ref, ids_ref, route_ref, gate_ref, gu_hbm, down_hbm) = (
        refs[:pairs], refs[pairs:2 * pairs], refs[2 * pairs:2 * pairs + 6]
    )
    refs = refs[2 * pairs + 6:]
    keep, send = refs[:pairs], refs[pairs:2 * pairs]
    x_ref, weight_ref, up_ref, down_ref, hidden_ref, sums_ref, sem = refs[2 * pairs:]
    span, columns = near[0].shape
    width = x_ref.shape[1]
    members = ys * halves
    group = lax.axis_index("dp")
    place = lax.axis_index("expert")
    up_copy = pltpu.make_async_copy(gu_hbm.at[0, 1], up_ref, sem.at[0])
    down_copy = pltpu.make_async_copy(down_hbm.at[0], down_ref, sem.at[1])
    up_copy.start()
    down_copy.start()

    groups = weight_ref.shape[0]
    tokens = ids_ref.shape[1]
    rows = tokens // groups
    zs = span // rows
    weight = jnp.sum(jnp.where(ids_ref[...] == group, route_ref[...], 0.0), axis=0, keepdims=True)
    weight = jnp.transpose(jnp.broadcast_to(weight, (8, tokens)))[:, :1]
    for g in range(groups):
        weight_ref[g] = weight[g * rows:(g + 1) * rows]

    for p in range(members):
        @pl.when(place == p)
        def _():
            for x in range(lo):
                for r in range(members):
                    j = p ^ r
                    blocks = far if r % halves else near
                    gain = gain_ref[:, j * columns:(j + 1) * columns]
                    v = blocks[x * ys + r // halves][...].astype(jnp.float32)
                    x_ref[x * span:(x + 1) * span, j * columns:(j + 1) * columns] = (v * gain).astype(jnp.bfloat16)

    x_all = x_ref[...]
    contract = (((1,), (1,)), ((), ()))
    gate = lax.dot_general(x_all, gate_ref[0], contract, preferred_element_type=jnp.float32)
    norms = []
    for x in range(lo):
        squares = jnp.zeros((span, columns), jnp.float32)
        for y in range(ys):
            for blocks in (near, far):
                v = blocks[x * ys + y][...].astype(jnp.float32)
                squares = squares + v * v
        norms.append(lax.rsqrt(jnp.sum(squares, axis=1, keepdims=True) / width + norm_eps))
    norm = jnp.concatenate(norms, axis=0)
    gate = gate * norm
    gate = gate * jax.nn.sigmoid(swish_alpha * gate)
    up_copy.wait()
    up = lax.dot_general(x_all, up_ref[...], contract, preferred_element_type=jnp.float32)
    hidden_ref[...] = ((up * norm + 1.0) * gate).astype(jnp.bfloat16)
    down_copy.wait()
    scale = jnp.concatenate([weight_ref[group ^ (z * lo + x)] for x in range(lo) for z in range(zs)], axis=0)
    hidden = hidden_ref[...]
    for i in range(0, width, 768):
        part = slice(i, min(i + 768, width))
        sums_ref[:, part] = (
            jnp.dot(hidden, down_ref[:, part], preferred_element_type=jnp.float32) * scale
        ).astype(jnp.bfloat16)
    for p in range(members):
        @pl.when(place == p)
        def _():
            for x in range(lo):
                for r in range(members):
                    j = p ^ r
                    blocks = send if r % halves else keep
                    blocks[x * ys + r // halves][...] = sums_ref[
                        x * span:(x + 1) * span, j * columns:(j + 1) * columns
                    ]


def expert_sums(near, far, norm_gain, expert_ids, route_weights, w_gate, w_gate_up, w_down, groups, lo):
    units, width = w_down.shape[1:]
    pairs = len(near)
    ys = pairs // lo
    span, columns = near[0].shape
    total = span * lo
    outs = pl.pallas_call(
        functools.partial(expert_kernel, lo=lo, ys=ys),
        out_shape=[jax.ShapeDtypeStruct((span, columns), jnp.bfloat16)] * (2 * pairs),
        in_specs=[VMEM] * (2 * pairs + 4) + [HBM] * 2,
        out_specs=[VMEM] * (2 * pairs),
        scratch_shapes=[
            pltpu.VMEM((total, width), jnp.bfloat16),
            pltpu.VMEM((groups, total // groups, 1), jnp.float32),
            pltpu.VMEM((units, width), jnp.bfloat16),
            pltpu.VMEM((units, width), jnp.bfloat16),
            pltpu.VMEM((total, units), jnp.bfloat16),
            pltpu.VMEM((total, width), jnp.bfloat16),
            pltpu.SemaphoreType.DMA((2,)),
        ],
        compiler_params=pltpu.CompilerParams(vmem_limit_bytes=36 * MIB),
        name="experts",
    )(
        *near, *far, norm_gain[None, :], expert_ids.T, route_weights.T, w_gate, in_hbm(w_gate_up), in_hbm(w_down)
    )
    return outs[:pairs], outs[pairs:]


def dense_body(
    queries, fresh_key, fresh_value, cached_keys, cached_values, lengths, sink_logit_rows, residual, o_weight,
    norm_gain, expert_ids, route_weights, w_gate_up, w_down
):
    groups = lax.axis_size("dp")
    members = lax.axis_size("expert")
    lo, halves = 2, 2
    zs, ys = groups // lo, members // halves
    rows = residual.shape[0]

    def swap(value, x=0, z=0, y=0, c=0):
        flip = (z * lo + x) * members + y * halves + c
        return lax.ppermute(value, ("dp", "expert"), [(i, i ^ flip) for i in range(groups * members)])

    attended, w_gate = attend_local(
        queries, fresh_key, fresh_value, cached_keys, cached_values, lengths, sink_logit_rows, w_gate_up
    )
    blocks = [attended]
    for r in range(1, members):
        blocks.append(swap(attended, y=r // halves, c=r % halves))
    o_weight = bring(attended, o_weight)
    stream = project(blocks, o_weight, residual)

    others = [(x, y) for x in range(lo) for y in range(ys)][1:]
    line = jnp.concatenate([stream] + [swap(stream, z=z) for z in range(1, zs)], axis=0)
    near = [line] + [swap(line, x=x, y=y) for x, y in others]
    far = [swap(block, c=1) for block in near]
    keep, send = expert_sums(near, far, norm_gain, expert_ids, route_weights, w_gate, w_gate_up, w_down, groups, lo)

    def added(parts):
        total = parts[0].astype(jnp.float32)
        for part in parts[1:]:
            total = total + part.astype(jnp.float32)
        return total

    def cut(value, i):
        return value[i * rows:(i + 1) * rows]

    chip = [added([keep[i], swap(send[i], c=1)]).astype(jnp.bfloat16) for i in range(3)]
    last, _ = lax.optimization_barrier((send[3], chip[1]))
    chip.append(added([keep[3], swap(last, c=1)]).astype(jnp.bfloat16))
    plane = added([chip[0], swap(chip[1], y=1), swap(chip[2], x=1)]).astype(jnp.bfloat16)
    corner = added([cut(chip[3], 0)] + [swap(cut(chip[3], z), z=z) for z in range(1, zs)]).astype(jnp.bfloat16)
    total = added([stream, cut(plane, 0)] + [swap(cut(plane, z), z=z) for z in range(1, zs)] + [swap(corner, x=1, y=1)])
    return total.astype(jnp.bfloat16)


def attend(queries, fresh_key, fresh_value, cached_keys, cached_values, lengths, sink_logit_rows):
    batch_count = queries.shape[0]
    head_groups = QUERY_HEADS // KEY_VALUE_HEADS
    query_head_rows = queries.reshape(batch_count, KEY_VALUE_HEADS, head_groups, HEAD_SIZE)
    key_rows = cached_keys.reshape(batch_count, WINDOW_LENGTH, KEY_VALUE_HEADS, HEAD_SIZE)
    value_rows = cached_values.reshape(batch_count, WINDOW_LENGTH, KEY_VALUE_HEADS, HEAD_SIZE)
    score_scale = 1.0 / math.sqrt(HEAD_SIZE)
    cache_scores = (
        jnp.einsum("bkgd,bwkd->bkgw", query_head_rows, key_rows, preferred_element_type=jnp.float32)
        * score_scale
    )
    own_scores = (
        jnp.einsum(
            "npwm,npm->npw",
            query_head_rows,
            fresh_key.reshape(batch_count, KEY_VALUE_HEADS, HEAD_SIZE),
            preferred_element_type=jnp.float32,
        )
        * score_scale
    )
    slots = jnp.arange(WINDOW_LENGTH, dtype=jnp.int32)
    valid = (slots[None, :] >= (WINDOW_LENGTH - lengths)[:, None])[:, None, None, :]
    sink_terms = sink_logit_rows.reshape(KEY_VALUE_HEADS, head_groups)[None]
    masked = jnp.where(valid, cache_scores, -jnp.inf)
    top = jnp.maximum(jnp.maximum(jnp.max(masked, axis=-1), own_scores), sink_terms)
    cache_exp = jnp.where(valid, jnp.exp(masked - top[..., None]), 0.0)
    self_exp = jnp.exp(own_scores - top)
    total = jnp.sum(cache_exp, axis=-1) + self_exp + jnp.exp(sink_terms - top)
    cache_prob = (cache_exp / total[..., None]).astype(jnp.bfloat16)
    own_probability = (self_exp / total).astype(jnp.bfloat16)
    blended = jnp.einsum(
        "bkgw,bwkd->bkgd", cache_prob, value_rows, preferred_element_type=jnp.float32
    )
    blended = blended + own_probability.astype(jnp.float32)[..., None] * fresh_value.reshape(
        batch_count, KEY_VALUE_HEADS, 1, HEAD_SIZE
    ).astype(jnp.float32)
    return blended.reshape(batch_count, QUERY_HEADS * HEAD_SIZE).astype(jnp.bfloat16)


def slot_onehot(named, capacity):
    counts = jnp.cumsum(named.astype(jnp.int32), axis=1) - 1
    places = jnp.arange(capacity, dtype=jnp.int32)
    return named[:, None, :] & (counts[:, None, :] == places[None, :, None])


def receiver_slots(expert_ids, route_weights, expert, blocks, capacity):
    picked = expert_ids == expert
    named = jnp.any(picked, axis=1).reshape(blocks, -1)
    weight_at = jnp.sum(jnp.where(picked, route_weights, 0.0), axis=1).reshape(blocks, -1)
    onehot = slot_onehot(named, capacity)
    slot_weight = jnp.sum(jnp.where(onehot, weight_at[:, None, :], 0.0), axis=2)
    return (onehot, slot_weight)


def sender_slots(my_ids, experts, capacity):
    labels = jnp.arange(experts, dtype=jnp.int32)
    named = jnp.any(my_ids[None, :, :] == labels[:, None, None], axis=2)
    return slot_onehot(named, capacity)


def body(
    queries,
    fresh_key,
    fresh_value,
    cached_keys,
    cached_values,
    lengths,
    sink_logit_rows,
    residual,
    o_weight,
    norm_gain,
    expert_ids,
    route_weights,
    w_gate_up,
    w_down,
):
    attended = attend(
        queries, fresh_key, fresh_value, cached_keys, cached_values, lengths, sink_logit_rows
    )
    projected = lax.dot_general(
        lax.all_gather(attended, "expert", axis=0, tiled=True),
        o_weight,
        (((1,), (1,)), ((), ())),
        preferred_element_type=jnp.float32,
    )
    stream = (residual.astype(jnp.float32) + projected).astype(jnp.bfloat16)
    wide = stream.astype(jnp.float32)
    group_rows = stream.shape[0]
    columns = stream.shape[1]
    experts = lax.axis_size("dp")
    capacity = 2 * group_rows * TOP // experts
    gain_cols = lax.dynamic_slice_in_dim(norm_gain, lax.axis_index("expert") * columns, columns)
    squares = lax.psum(jnp.sum(wide * wide, axis=1), "expert")
    score_scale = lax.rsqrt(squares / D + norm_eps)
    outgoing = (wide * score_scale[:, None] * gain_cols[None, :]).astype(jnp.bfloat16)
    _, slot_weight = receiver_slots(
        expert_ids, route_weights, lax.axis_index("dp"), experts, capacity
    )
    my_ids = lax.dynamic_slice_in_dim(expert_ids, lax.axis_index("dp") * group_rows, group_rows, 0)
    onehot_out = sender_slots(my_ids, experts, capacity)
    outbound = jnp.einsum(
        "ect,td->ecd", onehot_out.astype(jnp.bfloat16), outgoing, preferred_element_type=jnp.float32
    ).astype(jnp.bfloat16)
    received = lax.all_to_all(outbound, "dp", split_axis=0, concat_axis=0, tiled=True)
    rows = received.reshape(experts * capacity, columns)
    gate_up = w_gate_up[0]
    down = w_down[0]
    both = jnp.einsum(
        "rc,hfc->rhf",
        lax.all_gather(rows, "expert", axis=1, tiled=True),
        gate_up,
        preferred_element_type=jnp.float32,
    )
    gate = both[:, 0]
    up = both[:, 1]
    hidden = ((up + 1.0) * gate * jax.nn.sigmoid(swish_alpha * gate)).astype(jnp.bfloat16)
    summed = lax.psum_scatter(
        lax.dot_general(
            down, hidden, (((0,), (1,)), ((), ())), preferred_element_type=jnp.float32
        ).astype(jnp.bfloat16),
        "expert",
        scatter_dimension=0,
        tiled=True,
    ).astype(jnp.float32)
    contribution = (summed * slot_weight.reshape(1, -1)).astype(jnp.bfloat16)
    contribution = contribution.T.reshape(experts, capacity, columns)
    returned = lax.all_to_all(contribution, "dp", split_axis=0, concat_axis=0, tiled=True)
    returned_sum = jnp.einsum(
        "ect,ecd->td",
        onehot_out.astype(jnp.float32),
        returned.astype(jnp.float32),
        precision=lax.Precision.HIGHEST,
    )
    return (wide + returned_sum).astype(jnp.bfloat16)


def solution(mesh):
    placed = (
        P(("dp", "expert"), None),
        P(("dp", "expert"), None),
        P(("dp", "expert"), None),
        P(("dp", "expert"), None, None),
        P(("dp", "expert"), None, None),
        P(("dp", "expert")),
        P(),
        P("dp", "expert"),
        P("expert", None),
        P(),
        P(),
        P(),
        P("dp", None, "expert", None),
        P("dp", "expert", None),
    )

    def layer(*args):
        group_rows = args[7].shape[0]
        groups, members = mesh.shape["dp"], mesh.shape["expert"]
        capacity = 2 * group_rows * TOP // groups
        paired = groups & (groups - 1) == 0 and groups > 1 and members == 4
        return (dense_body if capacity >= group_rows and paired else body)(*args)

    return jax.shard_map(
        layer, mesh=mesh, in_specs=placed, out_specs=P("dp", "expert"), check_vma=False
    )
```

```python
import functools
import math

import jax
import jax.numpy as jnp
from jax import lax
from jax.experimental import pallas as pl
from jax.experimental.pallas import tpu as pltpu
from jax.sharding import PartitionSpec as P


D = 2880
QUERY_HEADS = 32
KEY_VALUE_HEADS = 4
HEAD_SIZE = 64
WINDOW_LENGTH = 128
TOP = 4


norm_eps = 1e-05
swish_alpha = 1.702
MIB = 1 << 20


def attend_kernel(
    len_hbm, sink_hbm, q_hbm, fk_hbm, fv_hbm, ck_hbm, cv_hbm, gu_hbm,
    out_ref, gu_ref, len_ref, sink_ref, q_ref, fk_ref, fv_ref, ck_ref, cv_ref, qs_ref, os_ref, sem
):
    ins = [
        (q_hbm, q_ref), (len_hbm, len_ref), (sink_hbm, sink_ref), (fk_hbm, fk_ref), (fv_hbm, fv_ref),
        (ck_hbm, ck_ref), (cv_hbm, cv_ref)
    ]
    ahead = [(gu_hbm.at[:, 0], gu_ref)]
    copies = [pltpu.make_async_copy(src, dst, sem.at[n]) for n, (src, dst) in enumerate(ins + ahead)]
    for copy in copies:
        copy.start()
    batch, width = q_ref.shape
    heads = sink_ref.shape[0]
    size = width // heads
    kv_heads = fk_ref.shape[1] // size
    group = heads // kv_heads
    window = ck_ref.shape[1]
    scale = 1.0 / math.sqrt(size)
    qs_ref[...] = jnp.zeros(qs_ref.shape, jnp.float32)
    slots = lax.broadcasted_iota(jnp.int32, (heads, window), 1)
    head_rows = lax.broadcasted_iota(jnp.int32, (heads, 1), 0)
    copies[0].wait()
    q = q_ref[...].astype(jnp.float32)
    for h in range(heads):
        k = h // group
        qs_ref[:, h, k * size:(k + 1) * size] = q[:, h * size:(h + 1) * size]
    for copy in copies[1:5]:
        copy.wait()
    sink = jnp.zeros((heads, 1), jnp.float32)
    for h in range(heads):
        sink = jnp.where(head_rows == h, sink_ref[h], sink)
    fk = fk_ref[...].astype(jnp.float32)
    fv = fv_ref[...].astype(jnp.float32)
    copies[5].wait()
    scores, owns = [], []
    for b in range(batch):
        qb = qs_ref[b]
        score = lax.dot_general(
            qb.astype(jnp.bfloat16), ck_ref[b], (((1,), (1,)), ((), ())), preferred_element_type=jnp.float32
        ) * scale
        scores.append(jnp.where(slots >= window - len_ref[b], score, -jnp.inf))
        owns.append(jnp.sum(qb * fk[b:b + 1], axis=1, keepdims=True) * scale)
    scores = jnp.concatenate(scores, axis=0)
    own = jnp.concatenate(owns, axis=0)
    sink = jnp.concatenate([sink] * batch, axis=0)
    top = jnp.maximum(jnp.maximum(jnp.max(scores, axis=1, keepdims=True), own), sink)
    probs = jnp.exp(scores - top)
    own = jnp.exp(own - top)
    total = jnp.sum(probs, axis=1, keepdims=True) + own + jnp.exp(sink - top)
    share = 1.0 / total
    probs = (probs * share).astype(jnp.bfloat16)
    own = (own * share).astype(jnp.bfloat16).astype(jnp.float32)
    copies[6].wait()
    for b in range(batch):
        part = slice(b * heads, (b + 1) * heads)
        os_ref[b] = jnp.dot(probs[part], cv_ref[b], preferred_element_type=jnp.float32) + own[part] * fv[b:b + 1]
    for h in range(0, heads, 2):
        k0 = h // group
        k1 = (h + 1) // group
        pair = jnp.concatenate(
            [os_ref[:, h, k0 * size:(k0 + 1) * size], os_ref[:, h + 1, k1 * size:(k1 + 1) * size]], axis=1
        )
        out_ref[:, h * size:(h + 2) * size] = pair.astype(jnp.bfloat16)
    for copy in copies[len(ins):]:
        copy.wait()


VMEM = pl.BlockSpec(memory_space=pltpu.VMEM)
SMEM = pl.BlockSpec(memory_space=pltpu.SMEM)
HBM = pl.BlockSpec(memory_space=pltpu.HBM)


def in_hbm(array):
    return pltpu.with_memory_space_constraint(array, pltpu.HBM)


def attend_local(
    queries, fresh_key, fresh_value, cached_keys, cached_values, lengths, sink_logit_rows, w_gate_up
):
    arrays = [queries, fresh_key, fresh_value, cached_keys, cached_values]
    small = [lengths, sink_logit_rows]
    spread = (queries.shape[0], sink_logit_rows.shape[0], fresh_key.shape[1])
    gate_shape = w_gate_up.shape[:1] + w_gate_up.shape[2:]
    return pl.pallas_call(
        attend_kernel,
        out_shape=[jax.ShapeDtypeStruct(shape, jnp.bfloat16) for shape in (queries.shape, gate_shape)],
        in_specs=[HBM] * 8,
        out_specs=[VMEM] * 2,
        scratch_shapes=[pltpu.SMEM(a.shape, a.dtype) for a in small] + [
            pltpu.VMEM(a.shape, a.dtype) for a in arrays
        ] + [
            pltpu.VMEM(spread, jnp.float32),
            pltpu.VMEM(spread, jnp.float32),
            pltpu.SemaphoreType.DMA((8,)),
        ],
        compiler_params=pltpu.CompilerParams(vmem_limit_bytes=32 * MIB),
        name="attend",
    )(*[in_hbm(a) for a in small + arrays + [w_gate_up]])


def bring_kernel(after_ref, source_hbm, target_ref, sem):
    copy = pltpu.make_async_copy(source_hbm, target_ref, sem.at[0])
    copy.start()
    copy.wait()


def bring(after, weight):
    call = pl.pallas_call(
        bring_kernel,
        out_shape=jax.ShapeDtypeStruct(weight.shape, weight.dtype),
        in_specs=[VMEM, HBM],
        out_specs=VMEM,
        scratch_shapes=[pltpu.SemaphoreType.DMA((1,))],
        compiler_params=pltpu.CompilerParams(vmem_limit_bytes=8 * MIB),
        cost_estimate=pl.CostEstimate(flops=10**9, bytes_accessed=4 * MIB, transcendentals=0),
        name="bring",
    )
    weight = in_hbm(weight)
    return call(after, weight)


def bring_experts_kernel(after_ref, gu_hbm, down_hbm, up_ref, down_ref, sem):
    copies = [
        pltpu.make_async_copy(gu_hbm.at[0, 1], up_ref, sem.at[0]),
        pltpu.make_async_copy(down_hbm.at[0], down_ref, sem.at[1]),
    ]
    for copy in copies:
        copy.start()
    for copy in copies:
        copy.wait()


def bring_experts(after, w_gate_up, w_down):
    call = pl.pallas_call(
        bring_experts_kernel,
        out_shape=[jax.ShapeDtypeStruct(w_down.shape[1:], w_down.dtype)] * 2,
        in_specs=[VMEM, HBM, HBM],
        out_specs=[VMEM] * 2,
        scratch_shapes=[pltpu.SemaphoreType.DMA((2,))],
        compiler_params=pltpu.CompilerParams(vmem_limit_bytes=12 * MIB),
        cost_estimate=pl.CostEstimate(flops=10**9, bytes_accessed=8 * MIB, transcendentals=0),
        name="bring_experts",
    )
    arrays = [in_hbm(w_gate_up), in_hbm(w_down)]
    return call(after, *arrays)


def project_kernel(*refs):
    blocks, (w_ref, res_ref, out_ref, rows_ref) = refs[:-4], refs[-4:]
    rows = blocks[0].shape[0]
    place = lax.axis_index("expert")
    for r, block in enumerate(blocks):
        rows_ref[pl.ds(pl.multiple_of((place ^ r) * rows, rows), rows), :] = block[...].astype(jnp.float32)
    projected = lax.dot_general(
        rows_ref[...].astype(jnp.bfloat16), w_ref[...], (((1,), (1,)), ((), ())), preferred_element_type=jnp.float32
    )
    out_ref[...] = (res_ref[...].astype(jnp.float32) + projected).astype(jnp.bfloat16)


def project(blocks, o_weight, residual):
    rows, width = blocks[0].shape
    return pl.pallas_call(
        project_kernel,
        out_shape=jax.ShapeDtypeStruct(residual.shape, jnp.bfloat16),
        in_specs=[VMEM] * (len(blocks) + 1) + [pl.BlockSpec(residual.shape, lambda: (0, 0))],
        out_specs=VMEM,
        scratch_shapes=[pltpu.VMEM((rows * len(blocks), width), jnp.float32)],
        compiler_params=pltpu.CompilerParams(vmem_limit_bytes=12 * MIB),
        name="project",
    )(*blocks, o_weight, residual)


def expert_kernel(*refs, lo, ys):
    halves = 2
    pairs = lo * ys
    near, far, (gain_ref, ids_ref, route_ref, gate_ref, up_ref, down_ref) = (
        refs[:pairs], refs[pairs:2 * pairs], refs[2 * pairs:2 * pairs + 6]
    )
    refs = refs[2 * pairs + 6:]
    keep, send = refs[:pairs], refs[pairs:2 * pairs]
    x_ref, weight_ref, hidden_ref, sums_ref = refs[2 * pairs:]
    span, columns = near[0].shape
    width = x_ref.shape[1]
    members = ys * halves
    group = lax.axis_index("dp")
    place = lax.axis_index("expert")

    groups = weight_ref.shape[0]
    tokens = ids_ref.shape[1]
    rows = tokens // groups
    zs = span // rows
    weight = jnp.sum(jnp.where(ids_ref[...] == group, route_ref[...], 0.0), axis=0, keepdims=True)
    weight = jnp.transpose(jnp.broadcast_to(weight, (8, tokens)))[:, :1]
    for g in range(groups):
        weight_ref[g] = weight[g * rows:(g + 1) * rows]

    for p in range(members):
        @pl.when(place == p)
        def _():
            for x in range(lo):
                for r in range(members):
                    j = p ^ r
                    blocks = far if r % halves else near
                    gain = gain_ref[:, j * columns:(j + 1) * columns]
                    v = blocks[x * ys + r // halves][...].astype(jnp.float32)
                    x_ref[x * span:(x + 1) * span, j * columns:(j + 1) * columns] = (v * gain).astype(jnp.bfloat16)

    x_all = x_ref[...]
    contract = (((1,), (1,)), ((), ()))
    gate = lax.dot_general(x_all, gate_ref[0], contract, preferred_element_type=jnp.float32)
    norms = []
    for x in range(lo):
        squares = jnp.zeros((span, columns), jnp.float32)
        for y in range(ys):
            for blocks in (near, far):
                v = blocks[x * ys + y][...].astype(jnp.float32)
                squares = squares + v * v
        norms.append(lax.rsqrt(jnp.sum(squares, axis=1, keepdims=True) / width + norm_eps))
    norm = jnp.concatenate(norms, axis=0)
    gate = gate * norm
    gate = gate * jax.nn.sigmoid(swish_alpha * gate)
    up = lax.dot_general(x_all, up_ref[...], contract, preferred_element_type=jnp.float32)
    hidden_ref[...] = ((up * norm + 1.0) * gate).astype(jnp.bfloat16)
    scale = jnp.concatenate([weight_ref[group ^ (z * lo + x)] for x in range(lo) for z in range(zs)], axis=0)
    hidden = hidden_ref[...]
    for i in range(0, width, 768):
        part = slice(i, min(i + 768, width))
        sums_ref[:, part] = (
            jnp.dot(hidden, down_ref[:, part], preferred_element_type=jnp.float32) * scale
        ).astype(jnp.bfloat16)
    for p in range(members):
        @pl.when(place == p)
        def _():
            for x in range(lo):
                for r in range(members):
                    j = p ^ r
                    blocks = send if r % halves else keep
                    blocks[x * ys + r // halves][...] = sums_ref[
                        x * span:(x + 1) * span, j * columns:(j + 1) * columns
                    ]


def expert_sums(near, far, norm_gain, expert_ids, route_weights, w_gate, w_up, w_down, groups, lo):
    units, width = w_down.shape
    pairs = len(near)
    ys = pairs // lo
    span, columns = near[0].shape
    total = span * lo
    outs = pl.pallas_call(
        functools.partial(expert_kernel, lo=lo, ys=ys),
        out_shape=[jax.ShapeDtypeStruct((span, columns), jnp.bfloat16)] * (2 * pairs),
        in_specs=[VMEM] * (2 * pairs + 6),
        out_specs=[VMEM] * (2 * pairs),
        scratch_shapes=[
            pltpu.VMEM((total, width), jnp.bfloat16),
            pltpu.VMEM((groups, total // groups, 1), jnp.float32),
            pltpu.VMEM((total, units), jnp.bfloat16),
            pltpu.VMEM((total, width), jnp.bfloat16),
        ],
        compiler_params=pltpu.CompilerParams(vmem_limit_bytes=24 * MIB),
        name="experts",
    )(
        *near, *far, norm_gain[None, :], expert_ids.T, route_weights.T, w_gate, w_up, w_down
    )
    return outs[:pairs], outs[pairs:]


def dense_body(
    queries, fresh_key, fresh_value, cached_keys, cached_values, lengths, sink_logit_rows, residual, o_weight,
    norm_gain, expert_ids, route_weights, w_gate_up, w_down
):
    groups = lax.axis_size("dp")
    members = lax.axis_size("expert")
    lo, halves = 2, 2
    zs = groups // lo
    rows = residual.shape[0]

    def swap(value, x=0, z=0, y=0, c=0):
        flip = (z * lo + x) * members + y * halves + c
        return lax.ppermute(value, ("dp", "expert"), [(i, i ^ flip) for i in range(groups * members)])

    attended, w_gate = attend_local(
        queries, fresh_key, fresh_value, cached_keys, cached_values, lengths, sink_logit_rows, w_gate_up
    )
    blocks = [attended]
    for r in range(1, members):
        blocks.append(swap(attended, y=r // halves, c=r % halves))
    o_weight = bring(attended, o_weight)
    stream = project(blocks, o_weight, residual)

    corner = swap(stream, x=1, y=1)
    line = jnp.concatenate([stream] + [swap(stream, z=z) for z in range(1, zs)], axis=0)
    spread = []
    for z in range(1, zs):
        spread.append(swap(corner, z=z))
    w_up, w_down = bring_experts(line, w_gate_up, w_down)
    near = [line, swap(line, y=1), swap(line, x=1), jnp.concatenate([corner] + spread, axis=0)]
    far = [swap(block, c=1) for block in near]
    keep, send = expert_sums(near, far, norm_gain, expert_ids, route_weights, w_gate, w_up, w_down, groups, lo)

    def added(parts):
        total = parts[0].astype(jnp.float32)
        for part in parts[1:]:
            total = total + part.astype(jnp.float32)
        return total

    def cut(value, i):
        return value[i * rows:(i + 1) * rows]

    chip = [added([keep[i], swap(send[i], c=1)]).astype(jnp.bfloat16) for i in range(3)]
    last, _ = lax.optimization_barrier((send[3], chip[1]))
    chip.append(added([keep[3], swap(last, c=1)]).astype(jnp.bfloat16))
    plane = added([chip[0], swap(chip[1], y=1), swap(chip[2], x=1)]).astype(jnp.bfloat16)
    corner = added([cut(chip[3], 0)] + [swap(cut(chip[3], z), z=z) for z in range(1, zs)]).astype(jnp.bfloat16)
    total = added([stream, cut(plane, 0)] + [swap(cut(plane, z), z=z) for z in range(1, zs)] + [swap(corner, x=1, y=1)])
    return total.astype(jnp.bfloat16)


def attend(queries, fresh_key, fresh_value, cached_keys, cached_values, lengths, sink_logit_rows):
    batch_count = queries.shape[0]
    head_groups = QUERY_HEADS // KEY_VALUE_HEADS
    query_head_rows = queries.reshape(batch_count, KEY_VALUE_HEADS, head_groups, HEAD_SIZE)
    key_rows = cached_keys.reshape(batch_count, WINDOW_LENGTH, KEY_VALUE_HEADS, HEAD_SIZE)
    value_rows = cached_values.reshape(batch_count, WINDOW_LENGTH, KEY_VALUE_HEADS, HEAD_SIZE)
    score_scale = 1.0 / math.sqrt(HEAD_SIZE)
    cache_scores = (
        jnp.einsum("bkgd,bwkd->bkgw", query_head_rows, key_rows, preferred_element_type=jnp.float32)
        * score_scale
    )
    own_scores = (
        jnp.einsum(
            "npwm,npm->npw",
            query_head_rows,
            fresh_key.reshape(batch_count, KEY_VALUE_HEADS, HEAD_SIZE),
            preferred_element_type=jnp.float32,
        )
        * score_scale
    )
    slots = jnp.arange(WINDOW_LENGTH, dtype=jnp.int32)
    valid = (slots[None, :] >= (WINDOW_LENGTH - lengths)[:, None])[:, None, None, :]
    sink_terms = sink_logit_rows.reshape(KEY_VALUE_HEADS, head_groups)[None]
    masked = jnp.where(valid, cache_scores, -jnp.inf)
    top = jnp.maximum(jnp.maximum(jnp.max(masked, axis=-1), own_scores), sink_terms)
    cache_exp = jnp.where(valid, jnp.exp(masked - top[..., None]), 0.0)
    self_exp = jnp.exp(own_scores - top)
    total = jnp.sum(cache_exp, axis=-1) + self_exp + jnp.exp(sink_terms - top)
    cache_prob = (cache_exp / total[..., None]).astype(jnp.bfloat16)
    own_probability = (self_exp / total).astype(jnp.bfloat16)
    blended = jnp.einsum(
        "bkgw,bwkd->bkgd", cache_prob, value_rows, preferred_element_type=jnp.float32
    )
    blended = blended + own_probability.astype(jnp.float32)[..., None] * fresh_value.reshape(
        batch_count, KEY_VALUE_HEADS, 1, HEAD_SIZE
    ).astype(jnp.float32)
    return blended.reshape(batch_count, QUERY_HEADS * HEAD_SIZE).astype(jnp.bfloat16)


def slot_onehot(named, capacity):
    counts = jnp.cumsum(named.astype(jnp.int32), axis=1) - 1
    places = jnp.arange(capacity, dtype=jnp.int32)
    return named[:, None, :] & (counts[:, None, :] == places[None, :, None])


def receiver_slots(expert_ids, route_weights, expert, blocks, capacity):
    picked = expert_ids == expert
    named = jnp.any(picked, axis=1).reshape(blocks, -1)
    weight_at = jnp.sum(jnp.where(picked, route_weights, 0.0), axis=1).reshape(blocks, -1)
    onehot = slot_onehot(named, capacity)
    slot_weight = jnp.sum(jnp.where(onehot, weight_at[:, None, :], 0.0), axis=2)
    return (onehot, slot_weight)


def sender_slots(my_ids, experts, capacity):
    labels = jnp.arange(experts, dtype=jnp.int32)
    named = jnp.any(my_ids[None, :, :] == labels[:, None, None], axis=2)
    return slot_onehot(named, capacity)


def body(
    queries,
    fresh_key,
    fresh_value,
    cached_keys,
    cached_values,
    lengths,
    sink_logit_rows,
    residual,
    o_weight,
    norm_gain,
    expert_ids,
    route_weights,
    w_gate_up,
    w_down,
):
    attended = attend(
        queries, fresh_key, fresh_value, cached_keys, cached_values, lengths, sink_logit_rows
    )
    projected = lax.dot_general(
        lax.all_gather(attended, "expert", axis=0, tiled=True),
        o_weight,
        (((1,), (1,)), ((), ())),
        preferred_element_type=jnp.float32,
    )
    stream = (residual.astype(jnp.float32) + projected).astype(jnp.bfloat16)
    wide = stream.astype(jnp.float32)
    group_rows = stream.shape[0]
    columns = stream.shape[1]
    experts = lax.axis_size("dp")
    capacity = 2 * group_rows * TOP // experts
    gain_cols = lax.dynamic_slice_in_dim(norm_gain, lax.axis_index("expert") * columns, columns)
    squares = lax.psum(jnp.sum(wide * wide, axis=1), "expert")
    score_scale = lax.rsqrt(squares / D + norm_eps)
    outgoing = (wide * score_scale[:, None] * gain_cols[None, :]).astype(jnp.bfloat16)
    _, slot_weight = receiver_slots(
        expert_ids, route_weights, lax.axis_index("dp"), experts, capacity
    )
    my_ids = lax.dynamic_slice_in_dim(expert_ids, lax.axis_index("dp") * group_rows, group_rows, 0)
    onehot_out = sender_slots(my_ids, experts, capacity)
    outbound = jnp.einsum(
        "ect,td->ecd", onehot_out.astype(jnp.bfloat16), outgoing, preferred_element_type=jnp.float32
    ).astype(jnp.bfloat16)
    received = lax.all_to_all(outbound, "dp", split_axis=0, concat_axis=0, tiled=True)
    rows = received.reshape(experts * capacity, columns)
    gate_up = w_gate_up[0]
    down = w_down[0]
    both = jnp.einsum(
        "rc,hfc->rhf",
        lax.all_gather(rows, "expert", axis=1, tiled=True),
        gate_up,
        preferred_element_type=jnp.float32,
    )
    gate = both[:, 0]
    up = both[:, 1]
    hidden = ((up + 1.0) * gate * jax.nn.sigmoid(swish_alpha * gate)).astype(jnp.bfloat16)
    summed = lax.psum_scatter(
        lax.dot_general(
            down, hidden, (((0,), (1,)), ((), ())), preferred_element_type=jnp.float32
        ).astype(jnp.bfloat16),
        "expert",
        scatter_dimension=0,
        tiled=True,
    ).astype(jnp.float32)
    contribution = (summed * slot_weight.reshape(1, -1)).astype(jnp.bfloat16)
    contribution = contribution.T.reshape(experts, capacity, columns)
    returned = lax.all_to_all(contribution, "dp", split_axis=0, concat_axis=0, tiled=True)
    returned_sum = jnp.einsum(
        "ect,ecd->td",
        onehot_out.astype(jnp.float32),
        returned.astype(jnp.float32),
        precision=lax.Precision.HIGHEST,
    )
    return (wide + returned_sum).astype(jnp.bfloat16)


def solution(mesh):
    placed = (
        P(("dp", "expert"), None),
        P(("dp", "expert"), None),
        P(("dp", "expert"), None),
        P(("dp", "expert"), None, None),
        P(("dp", "expert"), None, None),
        P(("dp", "expert")),
        P(),
        P("dp", "expert"),
        P("expert", None),
        P(),
        P(),
        P(),
        P("dp", None, "expert", None),
        P("dp", "expert", None),
    )

    def layer(*args):
        group_rows = args[7].shape[0]
        groups, members = mesh.shape["dp"], mesh.shape["expert"]
        capacity = 2 * group_rows * TOP // groups
        paired = groups & (groups - 1) == 0 and groups > 1 and members == 4
        return (dense_body if capacity >= group_rows and paired else body)(*args)

    return jax.shard_map(
        layer, mesh=mesh, in_specs=placed, out_specs=P("dp", "expert"), check_vma=False
    )
```
